32 devices in a mesh: row: 4 (over y, core), col: 8 (over z, x).
Axes of the slice: x: 2, y: 2, z: 4, core: 2. Of those that a mesh axis runs over, the one named last changes fastest.
Arguments:
- phase: float32 [512, 32, 512], P('col', 'row'), may hold values from -6 to 6
- velocity: float32 [3, 512, 32, 512], P(None, 'col', 'row'), may hold values from -12 to 12
Outputs:
- phase_next: float32 [512, 32, 512], P('col', 'row')
- velocity_next: float32 [3, 512, 32, 512], P(None, 'col', 'row')
The draws below stay inside these ranges and needn't reach their ends.
All inputs are finite; a program needn't handle non-finite values.
Results may differ from the reference program's by a relative error of at most 0.013.
Values may be sent and summed in bfloat16 or wider, within the bound.
A program may use at most 128 MiB of HBM per device.

```python
import math
import jax
import jax.numpy as jnp
from jax import lax

NX = 512
NY = 512
NZ = 32
KC = 192
KY = 384
KZH = 12
KZ = 24


def block_scale(rng, shape, cuts, low, largest):
    def one(dim, parts):
        heights = jax.random.uniform(jax.random.fold_in(jax.random.fold_in(rng, 6), dim), (parts,), jnp.float32, low / len(cuts), largest / len(cuts))
        return jnp.repeat(jnp.exp(heights), shape[dim] // parts).reshape((-1,) + (1,) * (len(shape) - dim - 1))

    factor_of = one(*cuts[0])
    for cut in cuts[1:]:
        factor_of = factor_of * one(*cut)
    return factor_of


def gaussian(key, extent, scale, reach, split=(), kind=jnp.bfloat16):
    gain = block_scale(key, extent, split, -0.22, 0.18) if split else 1.0
    drawn = jax.random.normal(key, extent, jnp.float32) * scale * gain
    return jnp.minimum(jnp.maximum(drawn, -reach), reach).astype(kind)


def setup_inputs(seed: int = 0) -> dict:
    key_of = jax.random.split(jax.random.key(seed), 3)
    return {
        "phase": gaussian(key_of[0], (NY, NZ, NX), 1.0, 6.0, ((0, 8), (1, 4)), jnp.float32),
        "velocity": gaussian(key_of[1], (3, NY, NZ, NX), 2.0, 12.0, ((1, 8), (2, 4)), jnp.float32),
    }


time_step = 1e-3
epsilon = 0.01
mobility = 1.0
reynolds = 100.0
stabilizer = 2.0


def cos_sin(row_index, col_index, period):
    residue = (row_index[:, None] * col_index[None, :]) % period
    angles = residue.astype(jnp.float32) * (2.0 * math.pi / period)
    return jnp.stack([jnp.cos(angles), jnp.sin(angles)]).astype(jnp.bfloat16)


def pair_sum(pieces, direction, stack_axis):
    if direction < 0:
        real_part = pieces[0, 0] + pieces[1, 1]
        imag_part = pieces[1, 0] - pieces[0, 1]
    else:
        real_part = pieces[0, 0] - pieces[1, 1]
        imag_part = pieces[0, 1] + pieces[1, 0]
    return jnp.stack([real_part, imag_part], axis=stack_axis)


def rounded(values):
    return lax.optimization_barrier(values.astype(jnp.bfloat16))


def product(form, first_op, second_op):
    return jnp.einsum(form, first_op.astype(jnp.float32), second_op.astype(jnp.float32), precision=lax.Precision.HIGHEST)


def times_i(values):
    return jnp.stack([-values[1], values[0]])


def reference(phase, velocity):
    table_x = cos_sin(jnp.arange(NX, dtype=jnp.int32), jnp.arange(KC, dtype=jnp.int32), NX)
    table_y = cos_sin(jnp.arange(NY, dtype=jnp.int32), jnp.arange(KY, dtype=jnp.int32) - KC, NY)
    table_z = cos_sin(jnp.arange(NZ, dtype=jnp.int32), jnp.arange(KZ, dtype=jnp.int32) - KZH, NZ)
    scale_inv = 1.0 / (NX * NY * NZ)
    weight = jnp.where(jnp.arange(KC) == 0, 1.0, 2.0).astype(jnp.float32)[:, None, None]

    def forward(field):
        pieces = product('yzx,txa->tayz', rounded(field), table_x)
        x_lines = rounded(jnp.stack([pieces[0], -pieces[1]]))
        pieces = product('payz,tyb->ptabz', x_lines, table_y)
        y_planes = rounded(pair_sum(pieces, -1, 0))
        pieces = product('pabz,tzm->ptabm', y_planes, table_z)
        return pair_sum(pieces, -1, 0) * scale_inv

    def inverse(coeff):
        pieces = product('pabm,tzm->ptabz', rounded(coeff), table_z)
        z_planes = rounded(pair_sum(pieces, 1, 0))
        pieces = product('pabz,tyb->ptayz', z_planes, table_y)
        x_lines = rounded(pair_sum(pieces, 1, 0))
        scaled = jnp.stack([x_lines[0] * weight, -(x_lines[1] * weight)])
        return product('payz,pxa->yzx', scaled, table_x)

    wave_x = jnp.arange(KC).astype(jnp.float32)[None, :, None, None]
    wave_y = (jnp.arange(KY) - KC).astype(jnp.float32)[None, None, :, None]
    wave_z = ((jnp.arange(KZ) - KZH).astype(jnp.float32) * (NX / NZ))[None, None, None, :]
    squared = wave_x * wave_x + wave_y * wave_y + wave_z * wave_z

    coeff_phase = forward(phase)
    coeff_u = [forward(velocity[j]) for j in range(3)]
    gradient = [inverse(times_i(wave_x * coeff_phase)), inverse(times_i(wave_y * coeff_phase)), inverse(times_i(wave_z * coeff_phase))]
    lap_field = inverse(-squared * coeff_phase)
    vortex = [inverse(times_i(wave_y * coeff_u[2] - wave_z * coeff_u[1])),
              inverse(times_i(wave_z * coeff_u[0] - wave_x * coeff_u[2])),
              inverse(times_i(wave_x * coeff_u[1] - wave_y * coeff_u[0]))]
    advect = velocity[0] * gradient[0] + velocity[1] * gradient[1] + velocity[2] * gradient[2]
    bulk_term = phase * phase * phase - phase
    potential = bulk_term - epsilon * epsilon * lap_field
    forcing = [velocity[1] * vortex[2] - velocity[2] * vortex[1] + potential * gradient[0],
               velocity[2] * vortex[0] - velocity[0] * vortex[2] + potential * gradient[1],
               velocity[0] * vortex[1] - velocity[1] * vortex[0] + potential * gradient[2]]
    mean_mode = (wave_x == 0) & (wave_y == 0) & (wave_z == 0)
    advect_hat = jnp.where(mean_mode, 0.0, forward(advect))
    bulk_hat = forward(bulk_term)
    force_hat = [forward(forcing[j]) for j in range(3)]
    stable_part = 1.0 / time_step + mobility * stabilizer * squared
    new_phase = (stable_part * coeff_phase - advect_hat - mobility * squared * bulk_hat) / (stable_part + mobility * epsilon * epsilon * squared * squared)
    viscous = 1.0 / time_step + squared / reynolds
    unprojected = [(coeff_u[j] / time_step + force_hat[j]) / viscous for j in range(3)]
    normal_part = (wave_x * unprojected[0] + wave_y * unprojected[1] + wave_z * unprojected[2]) / jnp.maximum(squared, 1.0)
    waves = [wave_x, wave_y, wave_z]
    phase_next = inverse(new_phase)
    velocity_next = jnp.stack([inverse(unprojected[j] - waves[j] * normal_part) for j in range(3)])
    return phase_next, velocity_next
```

```python
import math

import jax
import jax.numpy as jnp
import ml_dtypes
import numpy as np
from jax import lax
from jax.experimental import pallas as pl
from jax.experimental.pallas import tpu as pltpu
from jax.sharding import PartitionSpec as P

NX = 512
NY = 512
KC = 192
KY = 384


time_step = 0.001
epsilon = 0.01
mobility = 1.0
reynolds = 100.0
stabilizer = 2.0


def cos_sin(row_index, col_index, period):
    residue = row_index[:, None] * col_index[None, :] % period
    angles = residue.astype(jnp.float32) * (2.0 * math.pi / period)
    return jnp.stack([jnp.cos(angles), jnp.sin(angles)]).astype(jnp.bfloat16)


def pair_sum(pieces, direction, stack_axis):
    if direction < 0:
        real_part = pieces[0, 0] + pieces[1, 1]
        imag_part = pieces[1, 0] - pieces[0, 1]
    else:
        real_part = pieces[0, 0] - pieces[1, 1]
        imag_part = pieces[0, 1] + pieces[1, 0]
    return jnp.stack([real_part, imag_part], axis=stack_axis)


def times_i(values):
    return jnp.stack([-values[:, 1], values[:, 0]], axis=1)


def phase_terms(phase, velocity, gradient, lap_field):
    advect = velocity[0] * gradient[0] + velocity[1] * gradient[1] + velocity[2] * gradient[2]
    bulk_term = phase * phase * phase - phase
    potential = bulk_term - epsilon * epsilon * lap_field
    return (advect, bulk_term, potential)


def momentum(velocity, vortex, gradient, potential):
    return jnp.stack(
        [
            velocity[1] * vortex[2] - velocity[2] * vortex[1] + potential * gradient[0],
            velocity[2] * vortex[0] - velocity[0] * vortex[2] + potential * gradient[1],
            velocity[0] * vortex[1] - velocity[1] * vortex[0] + potential * gradient[2],
        ]
    )


def plain_device(phase, velocity):
    col_count = lax.axis_size("col")
    row_count = lax.axis_size("row")
    rows_y = phase.shape[0]
    planes = phase.shape[1]
    total_z = planes * row_count
    half_z = 3 * total_z // 8
    modes_z = 2 * half_z
    kx_local = KC // col_count
    ky_local = KY // row_count
    scale_inv = 1.0 / (NX * NY * total_z)
    table_x = cos_sin(jnp.arange(NX, dtype=jnp.int32), jnp.arange(KC, dtype=jnp.int32), NX)
    table_y = cos_sin(jnp.arange(NY, dtype=jnp.int32), jnp.arange(KY, dtype=jnp.int32) - KC, NY)
    table_z = cos_sin(
        jnp.arange(total_z, dtype=jnp.int32), jnp.arange(modes_z, dtype=jnp.int32) - half_z, total_z
    )
    y_forward = table_y.reshape(2, col_count, rows_y, KY)
    y_inverse = table_y.reshape(2, col_count, rows_y, row_count, ky_local)
    z_table = table_z.reshape(2, row_count, planes, modes_z)
    weight = jnp.where(jnp.arange(KC) == 0, 1.0, 2.0).astype(jnp.bfloat16)[:, None, None, None]

    def along_y(incoming):
        field_count = incoming.shape[1]
        shaped = incoming.reshape(incoming.shape[0], field_count, col_count, 2, rows_y, planes)
        pieces = jnp.einsum(
            "afcpyz,tcyb->ptafbz", shaped, y_forward, preferred_element_type=jnp.float32
        )
        joined = pair_sum(pieces, -1, 2).astype(jnp.bfloat16)
        return joined.reshape(incoming.shape[0], field_count, 2, KY * planes)

    def along_z(incoming):
        field_count = incoming.shape[1]
        shaped = incoming.reshape(incoming.shape[0], field_count, 2, row_count, ky_local, planes)
        pieces = jnp.einsum(
            "afprbz,trzm->ptafbm", shaped, z_table, preferred_element_type=jnp.float32
        )
        joined = pair_sum(pieces, -1, 2) * scale_inv
        return joined.reshape(incoming.shape[0], field_count, 2, ky_local * modes_z)

    def back_y(incoming):
        field_count = incoming.shape[1]
        shaped = incoming.reshape(incoming.shape[0], field_count, 2, row_count, planes, ky_local)
        pieces = jnp.einsum(
            "afprzb,tcyrb->ptafcyz", shaped, y_inverse, preferred_element_type=jnp.float32
        )
        joined = pair_sum(pieces, 1, 3).astype(jnp.bfloat16)
        return joined.reshape(incoming.shape[0], field_count, col_count * 2 * rows_y * planes)

    def back_x(incoming):
        field_count = incoming.shape[1]
        shaped = incoming.reshape(KC, field_count, 2, rows_y, planes)
        scaled = jnp.stack([shaped[:, :, 0] * weight, -(shaped[:, :, 1] * weight)], axis=2)
        return jnp.einsum("afpyz,pxa->fyzx", scaled, table_x, preferred_element_type=jnp.float32)

    def forward(fields):
        field_count = fields.shape[0]
        pieces = jnp.einsum(
            "fyzx,txa->tafyz",
            fields.astype(jnp.bfloat16),
            table_x,
            preferred_element_type=jnp.float32,
        )
        x_lines = jnp.stack([pieces[0], -pieces[1]], axis=2).astype(jnp.bfloat16)
        x_lines = x_lines.reshape(KC, field_count, 2 * rows_y * planes)
        spread = along_y(lax.all_to_all(x_lines, "col", split_axis=0, concat_axis=2, tiled=True))
        return along_z(lax.all_to_all(spread, "row", split_axis=3, concat_axis=3, tiled=True))

    def inverse(spectra):
        field_count = spectra.shape[1]
        shaped = spectra.astype(jnp.bfloat16).reshape(kx_local, field_count, 2, ky_local, modes_z)
        pieces = jnp.einsum(
            "afpbm,trzm->ptafrzb", shaped, z_table, preferred_element_type=jnp.float32
        )
        z_planes = (
            pair_sum(pieces, 1, 2)
            .astype(jnp.bfloat16)
            .reshape(kx_local, field_count, 2, total_z * ky_local)
        )
        spread = back_y(lax.all_to_all(z_planes, "row", split_axis=3, concat_axis=3, tiled=True))
        return back_x(lax.all_to_all(spread, "col", split_axis=2, concat_axis=0, tiled=True))

    spectra = forward(jnp.concatenate([phase[None], velocity], axis=0))
    wave_x = (lax.axis_index("col") * kx_local + jnp.arange(kx_local, dtype=jnp.int32)).astype(
        jnp.float32
    )[:, None, None]
    modes_y = lax.axis_index("row") * ky_local + jnp.arange(ky_local, dtype=jnp.int32) - KC
    wave_y = jnp.broadcast_to(modes_y.astype(jnp.float32)[:, None], (ky_local, modes_z)).reshape(-1)
    z_values = (jnp.arange(modes_z, dtype=jnp.int32) - half_z).astype(jnp.float32) * (NX / total_z)
    wave_z = jnp.broadcast_to(z_values[None, :], (ky_local, modes_z)).reshape(-1)
    squared = wave_x * wave_x + wave_y * wave_y + wave_z * wave_z
    coeff_phase = spectra[:, 0]
    coeff_u = spectra[:, 1]
    coeff_v = spectra[:, 2]
    coeff_w = spectra[:, 3]
    gradients = [
        times_i(wave_x * coeff_phase),
        times_i(wave_y * coeff_phase),
        times_i(wave_z * coeff_phase),
    ]
    laplace = -squared * coeff_phase
    vortex_hat = [
        times_i(wave_y * coeff_w - wave_z * coeff_v),
        times_i(wave_z * coeff_u - wave_x * coeff_w),
        times_i(wave_x * coeff_v - wave_y * coeff_u),
    ]
    leading = inverse(jnp.stack(gradients + [laplace], axis=1))
    advect, bulk_term, potential = phase_terms(phase, velocity, leading[0:3], leading[3])
    phase_side = forward(jnp.stack([advect, bulk_term]))
    vortex = inverse(jnp.stack(vortex_hat, axis=1))
    flow_side = forward(momentum(velocity, vortex, leading[0:3], potential))
    nonlinear = jnp.concatenate([phase_side, flow_side], axis=1)
    mean_mode = (wave_x == 0) & (wave_y == 0) & (wave_z == 0)
    advect_hat = jnp.where(mean_mode, 0.0, nonlinear[:, 0])
    bulk_hat = nonlinear[:, 1]
    stable_part = 1.0 / time_step + mobility * stabilizer * squared
    new_phase = (stable_part * coeff_phase - advect_hat - mobility * squared * bulk_hat) / (
        stable_part + mobility * epsilon * epsilon * squared * squared
    )
    viscous = 1.0 / time_step + squared / reynolds
    unprojected = [
        (spectra[:, 1 + j] / time_step + nonlinear[:, 2 + j]) / viscous for j in range(3)
    ]
    normal_part = (
        wave_x * unprojected[0] + wave_y * unprojected[1] + wave_z * unprojected[2]
    ) / jnp.maximum(squared, 1.0)
    waves = [wave_x, wave_y, wave_z]
    new_flow = [unprojected[j] - waves[j] * normal_part for j in range(3)]
    result = inverse(jnp.stack([new_phase] + new_flow, axis=1))
    return (result[0], result[1:4])


def tables(cols, rows, rows_y, planes):
    total_z = planes * rows
    half_z = 3 * total_z // 8
    modes_z = 2 * half_z
    kx_row = KC // rows

    def pair(first, second, period):
        residue = first[:, None] * second[None, :] % period
        angles = residue.astype(np.float32) * np.float32(2.0 * math.pi / period)
        return [np.cos(angles).astype(ml_dtypes.bfloat16), np.sin(angles).astype(ml_dtypes.bfloat16)]

    cos_x, sin_x = pair(np.arange(KC), np.arange(NX), NX)
    cos_y, sin_y = pair(np.arange(NY), np.arange(KY) - KC, NY)
    cos_z, sin_z = pair(np.arange(total_z), np.arange(modes_z) - half_z, total_z)
    x_table = np.stack([cos_x, -sin_x]).reshape(2, rows, kx_row // 2, 2, NX)
    x_table = x_table.transpose(1, 0, 3, 2, 4).reshape(2 * KC, NX)
    y_forward = np.concatenate([cos_y, sin_y], axis=1)
    y_inverse = np.concatenate([cos_y.T, sin_y.T], axis=1)
    cz, sz = (t.reshape(rows, planes, modes_z) for t in (cos_z, sin_z))
    z_forward = np.stack([np.stack([cz, sz], 1), np.stack([-sz, cz], 1)])
    z_forward = z_forward.transpose(0, 4, 1, 2, 3).reshape(2 * modes_z, 2 * total_z)
    z_inverse = np.stack([np.stack([cz, -sz], 2), np.stack([sz, cz], 2)], 1)
    z_inverse = z_inverse.reshape(2 * total_z, 2 * modes_z)
    z_rotated = np.concatenate([z_inverse[:, modes_z:], -z_inverse[:, :modes_z]], axis=1)
    made = (x_table, y_forward, y_inverse, z_forward, z_inverse, z_rotated)
    return [jnp.asarray(t.astype(ml_dtypes.bfloat16)) for t in made]


def dot(first, second, dims=((1,), (0,))):
    return lax.dot_general(first, second, (dims, ((), ())), preferred_element_type=jnp.float32)


LANES = 128


def fast_device(sizes, phase, velocity):
    cols, rows, rows_y, planes = sizes
    total_z = planes * rows
    half_z = 3 * total_z // 8
    modes_z = 2 * half_z
    kx_row = KC // rows
    kx_own = kx_row // cols
    pairs = kx_row // 2
    points = rows_y * planes
    row_lanes = kx_row * rows_y
    col_lanes = kx_own * rows_y
    own = kx_own * modes_z
    scale_inv = 1.0 / (NX * NY * total_z)
    made_tables = tables(cols, rows, rows_y, planes)
    f32, bf16 = jnp.float32, jnp.bfloat16
    forward_count, derived_count, derived_lines, final_count = 9, 7, 6, 4
    row_count = forward_count + derived_count + final_count
    col_count = forward_count + derived_lines + final_count

    def exchange(axis, size, src, dst, send, recv):
        me = lax.axis_index(axis)

        def copy(f, d):
            peer = lax.rem(me + d, size)
            return pltpu.make_async_remote_copy(
                src_ref=src.at[f, peer],
                dst_ref=dst.at[f, me],
                send_sem=send.at[f, d - 1],
                recv_sem=recv.at[f, d - 1],
                device_id={axis: peer},
                device_id_type=pl.DeviceIdType.MESH,
            )

        def start(f):
            for d in range(1, size):
                copy(f, d).start()
            dst[f, me] = src[f, me]

        def arrived(f):
            for d in range(1, size):
                copy(f, d).wait_recv()

        def sent(f):
            for d in range(1, size):
                copy(f, d).wait_send()

        return start, arrived, sent

    def greet():
        barrier = pltpu.get_barrier_semaphore()
        for axis, size in (("col", cols), ("row", rows)):
            for d in range(1, size):
                peer = lax.rem(lax.axis_index(axis) + d, size)
                pl.semaphore_signal(
                    barrier, inc=1, device_id={axis: peer}, device_id_type=pl.DeviceIdType.MESH
                )
        pl.semaphore_wait(barrier, cols + rows - 2)

    def swap_halves(first, second):
        half = LANES // 2
        low = jnp.concatenate([first[:, :half], second[:, :half]], axis=1)
        high = jnp.concatenate([first[:, half:], second[:, half:]], axis=1)
        return low, high

    def body(*refs):
        phase_in, flow_in = refs[:2]
        table_in = refs[2:8]
        phase_out, flow_out = refs[8:10]
        (
            row_src, row_dst, col_src, col_dst, fields, lines, derived, coeff, ready,
            x_tab, yf_tab, yi_tab, zf_tab, zi_tab, zr_tab,
            row_send, row_recv, col_send, col_recv, load_sem, table_sem, store_sem,
        ) = refs[10:]
        table_refs = (x_tab, yf_tab, yi_tab, zf_tab, zi_tab, zr_tab)
        row_start, row_arrived, row_sent = exchange("row", rows, row_src, row_dst, row_send, row_recv)
        col_start, col_arrived, col_sent = exchange("col", cols, col_src, col_dst, col_send, col_recv)

        def load(j, z):
            source = phase_in.at[:, z, :] if j == 0 else flow_in.at[j - 1, :, z, :]
            target = fields.at[j, pl.ds(z * rows_y, rows_y), :]
            return pltpu.make_async_copy(source, target, load_sem.at[j, z])

        def store(j, z):
            target = phase_out.at[:, z, :] if j == 0 else flow_out.at[j - 1, :, z, :]
            source = derived.at[j, pl.ds(z * rows_y, rows_y), :]
            return pltpu.make_async_copy(source, target, store_sem.at[j, z])

        def table_copy(k):
            return pltpu.make_async_copy(table_in[k], table_refs[k], table_sem.at[k])

        first_kx = lax.axis_index("row") * kx_row
        own_kx = first_kx + lax.axis_index("col") * kx_own

        def x_forward(f):
            made = dot(x_tab[...], lines[f], ((1,), (1,)))
            for r in range(rows):
                parts = []
                for p in range(2):
                    base = (r * 2 + p) * kx_row
                    even = made[base : base + pairs]
                    odd = made[base + pairs : base + kx_row]
                    planes_made = []
                    for j in range(planes // 2):
                        at = slice(j * LANES, (j + 1) * LANES)
                        planes_made.extend(swap_halves(even[:, at], odd[:, at]))
                    parts.append(jnp.swapaxes(jnp.stack(planes_made), 0, 1))
                both = jnp.concatenate(parts, axis=1).astype(bf16)
                for k in range(pairs):
                    row_src[f, r, :, k * LANES : (k + 1) * LANES] = both[k]
            row_start(f)

        def x_inverse(h):
            row_arrived(h)
            made = []
            for r in range(rows):
                whole_lines = row_dst[h, r].astype(f32)
                tiles = jnp.stack([whole_lines[:, k * LANES : (k + 1) * LANES] for k in range(pairs)])
                for p in range(2):
                    by_plane = jnp.swapaxes(tiles[:, p * planes : (p + 1) * planes], 0, 1)
                    even, odd = [], []
                    for j in range(planes // 2):
                        low, high = swap_halves(by_plane[2 * j], by_plane[2 * j + 1])
                        even.append(low)
                        odd.append(high)
                    made.append(jnp.concatenate(even, axis=1))
                    made.append(jnp.concatenate(odd, axis=1))
            gathered = jnp.concatenate(made, axis=0).astype(bf16)
            return dot(gathered, x_tab[...], ((0,), (0,)))

        def z_forward(f):
            row_arrived(f)
            stacked = row_dst[f].reshape(2 * total_z, row_lanes)
            made = dot(zf_tab[...], stacked).astype(bf16)
            for c in range(cols):
                col_src[f, c] = made[:, c * col_lanes : (c + 1) * col_lanes]
            col_start(f)

        def joined(g):
            return jnp.concatenate([col_dst[g, c] for c in range(cols)], axis=1)

        def row_emit(h, made):
            made = made.astype(bf16)
            for r in range(rows):
                row_src[h, r] = made[r * 2 * planes : (r + 1) * 2 * planes]
            row_start(h)

        def z_inverse(g, h):
            col_arrived(g)
            row_emit(h, dot(zi_tab[...], joined(g)))

        def y_forward(f):
            col_arrived(f)
            lhs = jnp.concatenate(
                [
                    jnp.concatenate(
                        [col_dst[f, c, :, a * rows_y : (a + 1) * rows_y] for c in range(cols)], axis=1
                    )
                    for a in range(kx_own)
                ],
                axis=0,
            )
            made = dot(lhs, yf_tab[...]).reshape(kx_own, 2 * modes_z, 2 * KY)
            first, second = made[:, :modes_z], made[:, modes_z:]
            real = first[:, :, :KY] + second[:, :, KY:]
            imag = second[:, :, :KY] - first[:, :, KY:]
            coeff[f, 0] = real.reshape(own, KY) * scale_inv
            coeff[f, 1] = imag.reshape(own, KY) * scale_inv

        def y_inverse(e):
            made = dot(ready[e], yi_tab[...])
            first, second = made[:own], made[own:]
            real = (first[:, :NY] - second[:, NY:]).reshape(kx_own, modes_z, NY)
            imag = (first[:, NY:] + second[:, :NY]).reshape(kx_own, modes_z, NY)
            both = jnp.concatenate([real, imag], axis=1).astype(bf16)
            g = e + forward_count
            for c in range(cols):
                col_src[g, c] = jnp.concatenate(
                    [both[a, :, c * rows_y : (c + 1) * rows_y] for a in range(kx_own)], axis=1
                )
            col_start(g)

        block = 2 * modes_z

        def spectral(work):
            def step(i, carry):
                base = pl.multiple_of(i * block, block)
                at = pl.ds(base, block)
                row = lax.broadcasted_iota(jnp.int32, (block, KY), 0)
                upper = row >= modes_z
                kx = own_kx + 2 * i + jnp.where(upper, 1, 0)
                kz = jnp.where(upper, row - modes_z, row) - half_z
                ky = lax.broadcasted_iota(jnp.int32, (block, KY), 1) - KC
                weight = jnp.where(kx == 0, 1.0, 2.0)
                mean_mode = (kx == 0) & (ky == 0) & (kz == 0)
                wx, wy = kx.astype(f32), ky.astype(f32)
                wz = kz.astype(f32) * (NX / total_z)
                k2 = wx * wx + wy * wy + wz * wz

                def get(f):
                    return coeff[f, 0, at, :], coeff[f, 1, at, :]

                def put(e, real, imag):
                    ready[e, at, :] = (real * weight).astype(bf16)
                    ready[e, pl.ds(pl.multiple_of(own + base, block), block), :] = (
                        imag * weight
                    ).astype(bf16)

                work(get, put, wx, wy, wz, k2, mean_mode)
                return carry

            lax.fori_loop(0, own // block, step, 0)

        def derive_phase(get, put, wx, wy, wz, k2, mean_mode):
            real, imag = get(0)
            put(0, real, imag)
            put(1, -(wy * imag), wy * real)
            put(2, -k2 * real, -k2 * imag)

        def derive_vortex(get, put, wx, wy, wz, k2, mean_mode):
            w = [wx, wy, wz]
            got = [get(1 + j) for j in range(3)]
            for e, j in ((3, 2), (4, 1), (5, 0)):
                p, q = (j + 1) % 3, (j + 2) % 3
                real = -(w[p] * got[q][1] - w[q] * got[p][1])
                put(e, real, w[p] * got[q][0] - w[q] * got[p][0])

        def solve_phase(get, put, wx, wy, wz, k2, mean_mode):
            old, bulk_hat, advect_hat = get(0), get(4), get(5)
            stable = 1.0 / time_step + mobility * stabilizer * k2
            below = stable + mobility * epsilon * epsilon * k2 * k2
            made = []
            for p in range(2):
                kept = jnp.where(mean_mode, 0.0, advect_hat[p])
                made.append((stable * old[p] - kept - mobility * k2 * bulk_hat[p]) / below)
            put(6, made[0], made[1])

        def solve_flow(get, put, wx, wy, wz, k2, mean_mode):
            viscous = 1.0 / time_step + k2 / reynolds
            largest = jnp.maximum(k2, 1.0)
            w = [wx, wy, wz]
            old = [get(1 + j) for j in range(3)]
            added = [get(6 + j) for j in range(3)]
            made = [[], [], []]
            for p in range(2):
                free = [(old[j][p] / time_step + added[j][p]) / viscous for j in range(3)]
                normal = (wx * free[0] + wy * free[1] + wz * free[2]) / largest
                for j in range(3):
                    made[j].append(free[j] - w[j] * normal)
            for j in range(3):
                put(7 + j, made[j][0], made[j][1])

        cut = 32

        def pointwise(work):
            def step(i, carry):
                work(pl.ds(pl.multiple_of(i * cut, cut), cut))
                return carry

            lax.fori_loop(0, points // cut, step, 0)

        def loop(begin, end, work):
            def step(i, carry):
                work(i)
                return carry

            lax.fori_loop(begin, end, step, 0)

        for z in range(planes):
            load(0, z).start()
        table_copy(0).start()
        for k in (3, 1, 2, 4, 5):
            table_copy(k).start()
        for j in range(1, 4):
            for z in range(planes):
                load(j, z).start()
        greet()

        def bring(f):
            def cast(at):
                lines[f, at, :] = fields[f, at, :].astype(bf16)

            pointwise(cast)
            x_forward(f)

        table_copy(0).wait()
        for j in range(4):
            for z in range(planes):
                load(j, z).wait()
        for k in range(1, 6):
            table_copy(k).wait()
        loop(0, 4, bring)

        def make_bulk(at):
            c = fields[0, at, :]
            lines[4, at, :] = (c * c * c - c).astype(bf16)

        pointwise(make_bulk)
        x_forward(4)
        loop(0, 4, z_forward)
        y_forward(0)
        spectral(derive_phase)
        loop(0, 3, y_inverse)
        loop(1, 4, y_forward)
        spectral(derive_vortex)
        loop(3, 6, y_inverse)
        z_forward(4)

        g0 = forward_count
        h0 = forward_count

        def phase_planes():
            col_arrived(g0)
            data = joined(g0)
            lane_kx = lax.broadcasted_iota(jnp.int32, (1, row_lanes), 1) // rows_y + first_kx
            row_emit(h0, dot(zr_tab[...], data) * lane_kx.astype(f32))
            row = lax.broadcasted_iota(jnp.int32, (2 * modes_z, 1), 0)
            kz = jnp.where(row >= modes_z, row - modes_z, row) - half_z
            scaled = (data.astype(f32) * (kz.astype(f32) * (NX / total_z))).astype(bf16)
            row_emit(h0 + 1, dot(zr_tab[...], scaled))

        def to_field(i):
            derived[i] = x_inverse(h0 + i)

        def make_advect(at):
            lines[5, at, :] = (
                fields[1, at, :] * derived[0, at, :]
                + fields[2, at, :] * derived[2, at, :]
                + fields[3, at, :] * derived[1, at, :]
            ).astype(bf16)

        gradient_at = (0, 2, 1)
        vortex_at = (6, 5, 4)

        def make_forcing(which):
            def work(at):
                c = fields[0, at, :]
                potential = c * c * c - c - epsilon * epsilon * derived[3, at, :]
                for j in which:
                    p, q = (j + 1) % 3, (j + 2) % 3
                    lines[6 + j, at, :] = (
                        fields[1 + p, at, :] * derived[vortex_at[q], at, :]
                        - fields[1 + q, at, :] * derived[vortex_at[p], at, :]
                        + potential * derived[gradient_at[j], at, :]
                    ).astype(bf16)

            return work

        phase_planes()
        z_inverse(g0 + 1, h0 + 2)
        loop(0, 2, to_field)
        z_inverse(g0 + 2, h0 + 3)
        to_field(2)
        pointwise(make_advect)
        x_forward(5)
        to_field(3)
        z_inverse(g0 + 3, h0 + 4)
        z_forward(5)
        to_field(4)
        z_inverse(g0 + 4, h0 + 5)
        to_field(5)
        pointwise(make_forcing((0,)))
        x_forward(6)
        z_inverse(g0 + 5, h0 + 6)
        z_forward(6)
        to_field(6)
        pointwise(make_forcing((1, 2)))
        loop(7, 9, x_forward)
        loop(4, 6, y_forward)
        spectral(solve_phase)
        y_inverse(6)
        loop(7, 9, z_forward)
        loop(6, 9, y_forward)
        spectral(solve_flow)
        loop(7, 10, y_inverse)

        g1 = forward_count + derived_lines
        h1 = forward_count + derived_count
        z_inverse(g1, h1)

        def finish(j):
            derived[j] = x_inverse(h1 + j)

        for j in range(final_count):
            if j + 1 < final_count:
                z_inverse(g1 + j + 1, h1 + j + 1)
            finish(j)
            for z in range(planes):
                store(j, z).start()
        loop(0, row_count, row_sent)
        loop(0, col_count, col_sent)
        for j in range(final_count):
            for z in range(planes):
                store(j, z).wait()

    sems = pltpu.SemaphoreType.DMA
    row_shape = (row_count, rows, 2 * planes, row_lanes)
    col_shape = (col_count, cols, 2 * modes_z, col_lanes)
    scratch = [
        pltpu.VMEM(row_shape, bf16),
        pltpu.VMEM(row_shape, bf16),
        pltpu.VMEM(col_shape, bf16),
        pltpu.VMEM(col_shape, bf16),
        pltpu.VMEM((4, points, NX), f32),
        pltpu.VMEM((forward_count, points, NX), bf16),
        pltpu.VMEM((derived_count, points, NX), f32),
        pltpu.VMEM((forward_count, 2, own, KY), f32),
        pltpu.VMEM((derived_lines + final_count, 2 * own, KY), bf16),
    ]
    scratch += [pltpu.VMEM(t.shape, bf16) for t in made_tables]
    scratch += [
        sems((row_count, rows - 1)),
        sems((row_count, rows - 1)),
        sems((col_count, cols - 1)),
        sems((col_count, cols - 1)),
        sems((4, planes)),
        sems((len(made_tables),)),
        sems((4, planes)),
    ]
    hbm = pl.BlockSpec(memory_space=pltpu.HBM)
    return tuple(
        pl.pallas_call(
            body,
            in_specs=[hbm] * (2 + len(made_tables)),
            out_specs=[hbm, hbm],
            out_shape=[
                jax.ShapeDtypeStruct(phase.shape, f32),
                jax.ShapeDtypeStruct(velocity.shape, f32),
            ],
            scratch_shapes=scratch,
            compiler_params=pltpu.CompilerParams(
                collective_id=0, has_side_effects=True, vmem_limit_bytes=67_043_328
            ),
            cost_estimate=pl.CostEstimate(
                flops=8_000_000_000, bytes_accessed=1 << 23, transcendentals=0
            ),
        )(phase, velocity, *made_tables)
    )


def solution(mesh):
    cols, rows = mesh.shape["col"], mesh.shape["row"]

    def on_device(phase, velocity):
        rows_y, planes = phase.shape[0], phase.shape[1]
        kx_own = KC // (rows * cols)
        modes_z = 2 * (3 * planes * rows // 8)
        aligned = planes == 8 and 2 * rows_y == LANES and cols % 2 == 0
        exact = KC == kx_own * rows * cols and kx_own % 2 == 0 and modes_z % 8 == 0
        if aligned and exact:
            return fast_device((cols, rows, rows_y, planes), phase, velocity)
        return plain_device(phase, velocity)

    return jax.shard_map(
        on_device,
        mesh=mesh,
        in_specs=(P("col", "row", None), P(None, "col", "row", None)),
        out_specs=(P("col", "row", None), P(None, "col", "row", None)),
        check_vma=False,
    )
```

```python
import math

import jax
import jax.numpy as jnp
import ml_dtypes
import numpy as np
from jax import lax
from jax.experimental import pallas as pl
from jax.experimental.pallas import tpu as pltpu
from jax.sharding import PartitionSpec as P

NX = 512
NY = 512
KC = 192
KY = 384


time_step = 0.001
epsilon = 0.01
mobility = 1.0
reynolds = 100.0
stabilizer = 2.0


def cos_sin(row_index, col_index, period):
    residue = row_index[:, None] * col_index[None, :] % period
    angles = residue.astype(jnp.float32) * (2.0 * math.pi / period)
    return jnp.stack([jnp.cos(angles), jnp.sin(angles)]).astype(jnp.bfloat16)


def pair_sum(pieces, direction, stack_axis):
    if direction < 0:
        real_part = pieces[0, 0] + pieces[1, 1]
        imag_part = pieces[1, 0] - pieces[0, 1]
    else:
        real_part = pieces[0, 0] - pieces[1, 1]
        imag_part = pieces[0, 1] + pieces[1, 0]
    return jnp.stack([real_part, imag_part], axis=stack_axis)


def times_i(values):
    return jnp.stack([-values[:, 1], values[:, 0]], axis=1)


def phase_terms(phase, velocity, gradient, lap_field):
    advect = velocity[0] * gradient[0] + velocity[1] * gradient[1] + velocity[2] * gradient[2]
    bulk_term = phase * phase * phase - phase
    potential = bulk_term - epsilon * epsilon * lap_field
    return (advect, bulk_term, potential)


def momentum(velocity, vortex, gradient, potential):
    return jnp.stack(
        [
            velocity[1] * vortex[2] - velocity[2] * vortex[1] + potential * gradient[0],
            velocity[2] * vortex[0] - velocity[0] * vortex[2] + potential * gradient[1],
            velocity[0] * vortex[1] - velocity[1] * vortex[0] + potential * gradient[2],
        ]
    )


def plain_device(phase, velocity):
    col_count = lax.axis_size("col")
    row_count = lax.axis_size("row")
    rows_y = phase.shape[0]
    planes = phase.shape[1]
    total_z = planes * row_count
    half_z = 3 * total_z // 8
    modes_z = 2 * half_z
    kx_local = KC // col_count
    ky_local = KY // row_count
    scale_inv = 1.0 / (NX * NY * total_z)
    table_x = cos_sin(jnp.arange(NX, dtype=jnp.int32), jnp.arange(KC, dtype=jnp.int32), NX)
    table_y = cos_sin(jnp.arange(NY, dtype=jnp.int32), jnp.arange(KY, dtype=jnp.int32) - KC, NY)
    table_z = cos_sin(
        jnp.arange(total_z, dtype=jnp.int32), jnp.arange(modes_z, dtype=jnp.int32) - half_z, total_z
    )
    y_forward = table_y.reshape(2, col_count, rows_y, KY)
    y_inverse = table_y.reshape(2, col_count, rows_y, row_count, ky_local)
    z_table = table_z.reshape(2, row_count, planes, modes_z)
    weight = jnp.where(jnp.arange(KC) == 0, 1.0, 2.0).astype(jnp.bfloat16)[:, None, None, None]

    def along_y(incoming):
        field_count = incoming.shape[1]
        shaped = incoming.reshape(incoming.shape[0], field_count, col_count, 2, rows_y, planes)
        pieces = jnp.einsum(
            "afcpyz,tcyb->ptafbz", shaped, y_forward, preferred_element_type=jnp.float32
        )
        joined = pair_sum(pieces, -1, 2).astype(jnp.bfloat16)
        return joined.reshape(incoming.shape[0], field_count, 2, KY * planes)

    def along_z(incoming):
        field_count = incoming.shape[1]
        shaped = incoming.reshape(incoming.shape[0], field_count, 2, row_count, ky_local, planes)
        pieces = jnp.einsum(
            "afprbz,trzm->ptafbm", shaped, z_table, preferred_element_type=jnp.float32
        )
        joined = pair_sum(pieces, -1, 2) * scale_inv
        return joined.reshape(incoming.shape[0], field_count, 2, ky_local * modes_z)

    def back_y(incoming):
        field_count = incoming.shape[1]
        shaped = incoming.reshape(incoming.shape[0], field_count, 2, row_count, planes, ky_local)
        pieces = jnp.einsum(
            "afprzb,tcyrb->ptafcyz", shaped, y_inverse, preferred_element_type=jnp.float32
        )
        joined = pair_sum(pieces, 1, 3).astype(jnp.bfloat16)
        return joined.reshape(incoming.shape[0], field_count, col_count * 2 * rows_y * planes)

    def back_x(incoming):
        field_count = incoming.shape[1]
        shaped = incoming.reshape(KC, field_count, 2, rows_y, planes)
        scaled = jnp.stack([shaped[:, :, 0] * weight, -(shaped[:, :, 1] * weight)], axis=2)
        return jnp.einsum("afpyz,pxa->fyzx", scaled, table_x, preferred_element_type=jnp.float32)

    def forward(fields):
        field_count = fields.shape[0]
        pieces = jnp.einsum(
            "fyzx,txa->tafyz",
            fields.astype(jnp.bfloat16),
            table_x,
            preferred_element_type=jnp.float32,
        )
        x_lines = jnp.stack([pieces[0], -pieces[1]], axis=2).astype(jnp.bfloat16)
        x_lines = x_lines.reshape(KC, field_count, 2 * rows_y * planes)
        spread = along_y(lax.all_to_all(x_lines, "col", split_axis=0, concat_axis=2, tiled=True))
        return along_z(lax.all_to_all(spread, "row", split_axis=3, concat_axis=3, tiled=True))

    def inverse(spectra):
        field_count = spectra.shape[1]
        shaped = spectra.astype(jnp.bfloat16).reshape(kx_local, field_count, 2, ky_local, modes_z)
        pieces = jnp.einsum(
            "afpbm,trzm->ptafrzb", shaped, z_table, preferred_element_type=jnp.float32
        )
        z_planes = (
            pair_sum(pieces, 1, 2)
            .astype(jnp.bfloat16)
            .reshape(kx_local, field_count, 2, total_z * ky_local)
        )
        spread = back_y(lax.all_to_all(z_planes, "row", split_axis=3, concat_axis=3, tiled=True))
        return back_x(lax.all_to_all(spread, "col", split_axis=2, concat_axis=0, tiled=True))

    spectra = forward(jnp.concatenate([phase[None], velocity], axis=0))
    wave_x = (lax.axis_index("col") * kx_local + jnp.arange(kx_local, dtype=jnp.int32)).astype(
        jnp.float32
    )[:, None, None]
    modes_y = lax.axis_index("row") * ky_local + jnp.arange(ky_local, dtype=jnp.int32) - KC
    wave_y = jnp.broadcast_to(modes_y.astype(jnp.float32)[:, None], (ky_local, modes_z)).reshape(-1)
    z_values = (jnp.arange(modes_z, dtype=jnp.int32) - half_z).astype(jnp.float32) * (NX / total_z)
    wave_z = jnp.broadcast_to(z_values[None, :], (ky_local, modes_z)).reshape(-1)
    squared = wave_x * wave_x + wave_y * wave_y + wave_z * wave_z
    coeff_phase = spectra[:, 0]
    coeff_u = spectra[:, 1]
    coeff_v = spectra[:, 2]
    coeff_w = spectra[:, 3]
    gradients = [
        times_i(wave_x * coeff_phase),
        times_i(wave_y * coeff_phase),
        times_i(wave_z * coeff_phase),
    ]
    laplace = -squared * coeff_phase
    vortex_hat = [
        times_i(wave_y * coeff_w - wave_z * coeff_v),
        times_i(wave_z * coeff_u - wave_x * coeff_w),
        times_i(wave_x * coeff_v - wave_y * coeff_u),
    ]
    leading = inverse(jnp.stack(gradients + [laplace], axis=1))
    advect, bulk_term, potential = phase_terms(phase, velocity, leading[0:3], leading[3])
    phase_side = forward(jnp.stack([advect, bulk_term]))
    vortex = inverse(jnp.stack(vortex_hat, axis=1))
    flow_side = forward(momentum(velocity, vortex, leading[0:3], potential))
    nonlinear = jnp.concatenate([phase_side, flow_side], axis=1)
    mean_mode = (wave_x == 0) & (wave_y == 0) & (wave_z == 0)
    advect_hat = jnp.where(mean_mode, 0.0, nonlinear[:, 0])
    bulk_hat = nonlinear[:, 1]
    stable_part = 1.0 / time_step + mobility * stabilizer * squared
    new_phase = (stable_part * coeff_phase - advect_hat - mobility * squared * bulk_hat) / (
        stable_part + mobility * epsilon * epsilon * squared * squared
    )
    viscous = 1.0 / time_step + squared / reynolds
    unprojected = [
        (spectra[:, 1 + j] / time_step + nonlinear[:, 2 + j]) / viscous for j in range(3)
    ]
    normal_part = (
        wave_x * unprojected[0] + wave_y * unprojected[1] + wave_z * unprojected[2]
    ) / jnp.maximum(squared, 1.0)
    waves = [wave_x, wave_y, wave_z]
    new_flow = [unprojected[j] - waves[j] * normal_part for j in range(3)]
    result = inverse(jnp.stack([new_phase] + new_flow, axis=1))
    return (result[0], result[1:4])


def tables(cols, rows, rows_y, planes):
    total_z = planes * rows
    half_z = 3 * total_z // 8
    modes_z = 2 * half_z
    kx_row = KC // rows

    def pair(first, second, period):
        residue = first[:, None] * second[None, :] % period
        angles = residue.astype(np.float32) * np.float32(2.0 * math.pi / period)
        return [np.cos(angles).astype(ml_dtypes.bfloat16), np.sin(angles).astype(ml_dtypes.bfloat16)]

    cos_x, sin_x = pair(np.arange(KC), np.arange(NX), NX)
    cos_y, sin_y = pair(np.arange(NY), np.arange(KY) - KC, NY)
    cos_z, sin_z = pair(np.arange(total_z), np.arange(modes_z) - half_z, total_z)
    order = np.arange(KC).reshape(cols, rows, kx_row // cols).transpose(1, 0, 2).reshape(KC)
    x_table = np.stack([cos_x[order], -sin_x[order]]).reshape(2, rows, kx_row // 2, 2, NX)
    x_table = x_table.transpose(1, 0, 3, 2, 4).reshape(2 * KC, NX)
    y_forward = np.concatenate([cos_y, sin_y], axis=1)
    cz, sz = (t.reshape(rows, planes, modes_z) for t in (cos_z, sin_z))
    z_forward = np.stack([np.stack([cz, sz], 1), np.stack([-sz, cz], 1)])
    z_forward = z_forward.transpose(0, 4, 1, 2, 3).reshape(2 * modes_z, 2 * total_z)
    z_inverse = np.stack([np.stack([cz, -sz], 2), np.stack([sz, cz], 2)], 1)
    z_inverse = z_inverse.reshape(2 * total_z, 2 * modes_z)
    z_rotated = np.concatenate([z_inverse[:, modes_z:], -z_inverse[:, :modes_z]], axis=1)
    made = (x_table, y_forward, z_forward, z_inverse, z_rotated)
    return [jnp.asarray(t.astype(ml_dtypes.bfloat16)) for t in made]


def dot(first, second, dims=((1,), (0,))):
    return lax.dot_general(first, second, (dims, ((), ())), preferred_element_type=jnp.float32)


LANES = 128


def fast_device(sizes, phase, velocity):
    cols, rows, rows_y, planes = sizes
    total_z = planes * rows
    half_z = 3 * total_z // 8
    modes_z = 2 * half_z
    kx_row = KC // rows
    kx_own = kx_row // cols
    pairs = kx_row // 2
    points = rows_y * planes
    row_lanes = kx_row * rows_y
    col_lanes = kx_own * rows_y
    own = kx_own * modes_z
    scale_inv = 1.0 / (NX * NY * total_z)
    made_tables = tables(cols, rows, rows_y, planes)
    f32, bf16 = jnp.float32, jnp.bfloat16
    forward_count, derived_count, derived_lines, final_count = 8, 7, 6, 3
    row_count = forward_count + derived_count
    col_count = forward_count + derived_lines
    kx_col = kx_own * rows
    wide_lanes = kx_own * KY

    def exchange(axis, size, src, dst, send, recv):
        me = lax.axis_index(axis)

        def copy(f, d):
            peer = lax.rem(me + d, size)
            return pltpu.make_async_remote_copy(
                src_ref=src.at[f, peer],
                dst_ref=dst.at[f, me],
                send_sem=send.at[f, d - 1],
                recv_sem=recv.at[f, d - 1],
                device_id={axis: peer},
                device_id_type=pl.DeviceIdType.MESH,
            )

        def start(f):
            for d in range(1, size):
                copy(f, d).start()
            dst[f, me] = src[f, me]

        def arrived(f):
            for d in range(1, size):
                copy(f, d).wait_recv()

        def sent(f):
            for d in range(1, size):
                copy(f, d).wait_send()

        return start, arrived, sent

    def greet():
        barrier = pltpu.get_barrier_semaphore()
        for axis, size in (("col", cols), ("row", rows)):
            for d in range(1, size):
                peer = lax.rem(lax.axis_index(axis) + d, size)
                pl.semaphore_signal(
                    barrier, inc=1, device_id={axis: peer}, device_id_type=pl.DeviceIdType.MESH
                )

    def greeted():
        pl.semaphore_wait(pltpu.get_barrier_semaphore(), cols + rows - 2)

    def swap_halves(first, second):
        half = LANES // 2
        low = jnp.concatenate([first[:, :half], second[:, :half]], axis=1)
        high = jnp.concatenate([first[:, half:], second[:, half:]], axis=1)
        return low, high

    def body(*refs):
        phase_in, flow_in = refs[:2]
        table_in = refs[2:7]
        phase_out, flow_out = refs[7:9]
        (
            row_src, row_dst, col_src, col_dst, thin_src, thin_dst, wide_src, wide_dst,
            fields, lines, derived, coeff, ready,
            x_tab, yf_tab, zf_tab, zi_tab, zr_tab, xw_tab, yi_tab,
            row_send, row_recv, col_send, col_recv, thin_send, thin_recv, wide_send, wide_recv,
            load_sem, table_sem, store_sem,
        ) = refs[9:]
        table_refs = (x_tab, yf_tab, zf_tab, zi_tab, zr_tab)
        row_start, row_arrived, row_sent = exchange("row", rows, row_src, row_dst, row_send, row_recv)
        col_start, col_arrived, col_sent = exchange("col", cols, col_src, col_dst, col_send, col_recv)
        thin_start, thin_arrived, thin_sent = exchange(
            "row", rows, thin_src, thin_dst, thin_send, thin_recv
        )
        wide_start, wide_arrived, wide_sent = exchange(
            "col", cols, wide_src, wide_dst, wide_send, wide_recv
        )

        def load(j, z):
            source = phase_in.at[:, z, :] if j == 0 else flow_in.at[j - 1, :, z, :]
            target = fields.at[j, pl.ds(z * rows_y, rows_y), :]
            return pltpu.make_async_copy(source, target, load_sem.at[j, z])

        def store(j, z):
            target = phase_out.at[:, z, :] if j == 0 else flow_out.at[j - 1, :, z, :]
            source = derived.at[j, pl.ds(z * rows_y, rows_y), :]
            return pltpu.make_async_copy(source, target, store_sem.at[j, z])

        def table_copy(k):
            return pltpu.make_async_copy(table_in[k], table_refs[k], table_sem.at[k])

        row_kx = lax.axis_index("row") * kx_own
        own_kx = lax.axis_index("col") * kx_col + row_kx

        def x_forward(f):
            made = dot(x_tab[...], lines[lax.rem(f, 5)], ((1,), (1,)))
            for r in range(rows):
                parts = []
                for p in range(2):
                    base = (r * 2 + p) * kx_row
                    even = made[base : base + pairs]
                    odd = made[base + pairs : base + kx_row]
                    planes_made = []
                    for j in range(planes // 2):
                        at = slice(j * LANES, (j + 1) * LANES)
                        planes_made.extend(swap_halves(even[:, at], odd[:, at]))
                    parts.append(jnp.swapaxes(jnp.stack(planes_made), 0, 1))
                both = jnp.concatenate(parts, axis=1).astype(bf16)
                for k in range(pairs):
                    row_src[f - 1, r, :, k * LANES : (k + 1) * LANES] = both[k]
            row_start(f - 1)

        def x_inverse(h):
            row_arrived(h)
            made = []
            for r in range(rows):
                whole_lines = row_dst[h, r].astype(f32)
                tiles = jnp.stack([whole_lines[:, k * LANES : (k + 1) * LANES] for k in range(pairs)])
                for p in range(2):
                    by_plane = jnp.swapaxes(tiles[:, p * planes : (p + 1) * planes], 0, 1)
                    even, odd = [], []
                    for j in range(planes // 2):
                        low, high = swap_halves(by_plane[2 * j], by_plane[2 * j + 1])
                        even.append(low)
                        odd.append(high)
                    made.append(jnp.concatenate(even, axis=1))
                    made.append(jnp.concatenate(odd, axis=1))
            gathered = jnp.concatenate(made, axis=0).astype(bf16)
            return dot(gathered, x_tab[...], ((0,), (0,)))

        def z_forward(f):
            row_arrived(f - 1)
            stacked = row_dst[f - 1].reshape(2 * total_z, row_lanes)
            made = dot(zf_tab[...], stacked).astype(bf16)
            for c in range(cols):
                col_src[f - 1, c] = made[:, c * col_lanes : (c + 1) * col_lanes]
            col_start(f - 1)

        def joined(g):
            return jnp.concatenate([col_dst[g, c] for c in range(cols)], axis=1)

        def row_emit(h, made):
            made = made.astype(bf16)
            for r in range(rows):
                row_src[h, r] = made[r * 2 * planes : (r + 1) * 2 * planes]
            row_start(h)

        def wide_tables():
            out_row = lax.broadcasted_iota(jnp.int32, (2 * KC, 2 * KC), 0)
            in_row = lax.broadcasted_iota(jnp.int32, (2 * KC, 2 * KC), 1)
            c = out_row // (2 * kx_col)
            inside = out_row - c * 2 * kx_col
            part = jnp.where(inside >= kx_col, 1, 0)
            kx = inside - part * kx_col
            r = kx // kx_own
            a = c * kx_own + kx - r * kx_own
            wanted = (2 * r + part) * kx_row + (a % 2) * pairs + a // 2
            chosen = jnp.where(in_row == wanted, 1.0, 0.0).astype(bf16)
            xw_tab[...] = dot(chosen, x_tab[...]).astype(bf16)

        def inverse_table():
            for t in range(2):
                part = yf_tab[:, t * KY : (t + 1) * KY].astype(f32)
                yi_tab[:, t * NY : (t + 1) * NY] = part.T.astype(bf16)

        def first_x():
            made = dot(xw_tab[...], lines[0], ((1,), (1,))).astype(bf16)
            wide_src[0] = made.reshape(cols, 2 * kx_col, points)

        def first_y():
            wide_arrived(0)
            lhs = jnp.concatenate(
                [
                    jnp.concatenate(
                        [wide_dst[0, c, :, z * rows_y : (z + 1) * rows_y] for c in range(cols)], axis=1
                    )
                    for z in range(planes)
                ],
                axis=0,
            )
            made = dot(lhs, yf_tab[...]).reshape(planes, 2 * kx_col, 2 * KY)
            first, second = made[:, :kx_col], made[:, kx_col:]
            real = jnp.swapaxes(first[:, :, :KY] + second[:, :, KY:], 0, 1)
            imag = jnp.swapaxes(second[:, :, :KY] - first[:, :, KY:], 0, 1)
            both = jnp.concatenate([real, imag], axis=1).astype(bf16)
            for k in range(kx_col):
                r, a = k // kx_own, k % kx_own
                thin_src[0, r, :, a * KY : (a + 1) * KY] = both[k]
            thin_start(0)

        def first_z():
            thin_arrived(0)
            stacked = thin_dst[0].reshape(2 * total_z, wide_lanes)
            made = dot(zf_tab[...], stacked) * scale_inv
            for p in range(2):
                for a in range(kx_own):
                    coeff[0, p, a * modes_z : (a + 1) * modes_z, :] = made[
                        p * modes_z : (p + 1) * modes_z, a * KY : (a + 1) * KY
                    ]

        def last_z():
            parts = []
            for p in range(2):
                parts.append(
                    jnp.concatenate(
                        [coeff[0, p, a * modes_z : (a + 1) * modes_z, :] for a in range(kx_own)], axis=1
                    )
                )
            made = dot(zi_tab[...], jnp.concatenate(parts, axis=0).astype(bf16)).astype(bf16)
            for r in range(rows):
                thin_src[0, r] = made[r * 2 * planes : (r + 1) * 2 * planes]
            thin_start(0)

        def last_y():
            thin_arrived(0)
            lhs = jnp.concatenate(
                [
                    thin_dst[0, r, :, a * KY : (a + 1) * KY]
                    for r in range(rows)
                    for a in range(kx_own)
                ],
                axis=0,
            )
            made = dot(lhs, yi_tab[...]).reshape(kx_col, 2 * planes, 2 * NY)
            first, second = made[:, :planes], made[:, planes:]
            real = jnp.swapaxes(first[:, :, :NY] - second[:, :, NY:], 0, 1)
            imag = jnp.swapaxes(first[:, :, NY:] + second[:, :, :NY], 0, 1)
            both = jnp.concatenate([real, imag], axis=1).astype(bf16)
            for c in range(cols):
                wide_src[0, c] = jnp.concatenate(
                    [both[z, :, c * rows_y : (c + 1) * rows_y] for z in range(planes)], axis=1
                )
            wide_start(0)

        def last_x():
            wide_arrived(0)
            gathered = wide_dst[0].reshape(2 * KC, points)
            return dot(gathered, xw_tab[...], ((0,), (0,)))

        def z_inverse(g, h):
            col_arrived(g)
            row_emit(h, dot(zi_tab[...], joined(g)))

        def y_forward(f):
            col_arrived(f - 1)
            lhs = jnp.concatenate(
                [
                    jnp.concatenate(
                        [col_dst[f - 1, c, :, a * rows_y : (a + 1) * rows_y] for c in range(cols)], axis=1
                    )
                    for a in range(kx_own)
                ],
                axis=0,
            )
            made = dot(lhs, yf_tab[...]).reshape(kx_own, 2 * modes_z, 2 * KY)
            first, second = made[:, :modes_z], made[:, modes_z:]
            real = first[:, :, :KY] + second[:, :, KY:]
            imag = second[:, :, :KY] - first[:, :, KY:]
            coeff[f, 0] = real.reshape(own, KY) * scale_inv
            coeff[f, 1] = imag.reshape(own, KY) * scale_inv

        def y_inverse(e, g):
            made = dot(ready[e], yi_tab[...])
            first, second = made[:own], made[own:]
            real = (first[:, :NY] - second[:, NY:]).reshape(kx_own, modes_z, NY)
            imag = (first[:, NY:] + second[:, :NY]).reshape(kx_own, modes_z, NY)
            both = jnp.concatenate([real, imag], axis=1).astype(bf16)
            for c in range(cols):
                col_src[g, c] = jnp.concatenate(
                    [both[a, :, c * rows_y : (c + 1) * rows_y] for a in range(kx_own)], axis=1
                )
            col_start(g)

        block = 2 * modes_z

        def spectral(work):
            def step(i, carry):
                base = pl.multiple_of(i * block, block)
                at = pl.ds(base, block)
                row = lax.broadcasted_iota(jnp.int32, (block, KY), 0)
                upper = row >= modes_z
                kx = own_kx + 2 * i + jnp.where(upper, 1, 0)
                kz = jnp.where(upper, row - modes_z, row) - half_z
                ky = lax.broadcasted_iota(jnp.int32, (block, KY), 1) - KC
                weight = jnp.where(kx == 0, 1.0, 2.0)
                mean_mode = (kx == 0) & (ky == 0) & (kz == 0)
                wx, wy = kx.astype(f32), ky.astype(f32)
                wz = kz.astype(f32) * (NX / total_z)
                k2 = wx * wx + wy * wy + wz * wz

                def get(f):
                    return coeff[f, 0, at, :], coeff[f, 1, at, :]

                def put(e, real, imag):
                    if e is None:
                        coeff[0, 0, at, :] = real * weight
                        coeff[0, 1, at, :] = imag * weight
                        return
                    ready[e, at, :] = (real * weight).astype(bf16)
                    ready[e, pl.ds(pl.multiple_of(own + base, block), block), :] = (
                        imag * weight
                    ).astype(bf16)

                work(get, put, wx, wy, wz, k2, mean_mode)
                return carry

            lax.fori_loop(0, own // block, step, 0)

        def derive_phase(get, put, wx, wy, wz, k2, mean_mode):
            real, imag = get(0)
            put(0, real, imag)
            put(1, -(wy * imag), wy * real)
            put(2, -k2 * real, -k2 * imag)

        def derive_vortex(get, put, wx, wy, wz, k2, mean_mode):
            w = [wx, wy, wz]
            got = [get(1 + j) for j in range(3)]
            for e, j in ((3, 2), (4, 1), (5, 0)):
                p, q = (j + 1) % 3, (j + 2) % 3
                real = -(w[p] * got[q][1] - w[q] * got[p][1])
                put(e, real, w[p] * got[q][0] - w[q] * got[p][0])

        def solve_phase(get, put, wx, wy, wz, k2, mean_mode):
            old, bulk_hat, advect_hat = get(0), get(4), get(5)
            stable = 1.0 / time_step + mobility * stabilizer * k2
            below = stable + mobility * epsilon * epsilon * k2 * k2
            made = []
            for p in range(2):
                kept = jnp.where(mean_mode, 0.0, advect_hat[p])
                made.append((stable * old[p] - kept - mobility * k2 * bulk_hat[p]) / below)
            put(0, made[0], made[1])

        def solve_flow(get, put, wx, wy, wz, k2, mean_mode):
            viscous = 1.0 / time_step + k2 / reynolds
            largest = jnp.maximum(k2, 1.0)
            w = [wx, wy, wz]
            old = [get(1 + j) for j in range(3)]
            added = [get(6 + j) for j in range(3)]
            made = [[], [], []]
            for p in range(2):
                free = [(old[j][p] / time_step + added[j][p]) / viscous for j in range(3)]
                normal = (wx * free[0] + wy * free[1] + wz * free[2]) / largest
                for j in range(3):
                    made[j].append(free[j] - w[j] * normal)
            for j in range(3):
                put(1 + j if j < 2 else None, made[j][0], made[j][1])

        cut = 32

        def pointwise(work):
            def step(i, carry):
                work(pl.ds(pl.multiple_of(i * cut, cut), cut))
                return carry

            lax.fori_loop(0, points // cut, step, 0)

        def loop(begin, end, work):
            def step(i, carry):
                work(i)
                return carry

            lax.fori_loop(begin, end, step, 0)

        for z in range(planes):
            load(0, z).start()
        for k in range(len(table_refs)):
            table_copy(k).start()
        for j in range(1, 4):
            for z in range(planes):
                load(j, z).start()
        greet()

        def cast(f):
            def work(at):
                lines[f, at, :] = fields[f, at, :].astype(bf16)

            pointwise(work)

        def bring(f):
            for z in range(planes):
                load(f, z).wait()
            cast(f)

        def make_bulk(at):
            c = fields[0, at, :]
            lines[4, at, :] = (c * c * c - c).astype(bf16)

        def send_derived(e):
            y_inverse(e, forward_count + e)

        table_copy(0).wait()
        wide_tables()
        bring(0)
        first_x()
        greeted()
        wide_start(0)
        for j in range(1, 4):
            bring(j)
        loop(1, 4, x_forward)
        for k in range(1, len(table_refs)):
            table_copy(k).wait()
        inverse_table()
        pointwise(make_bulk)
        loop(1, 3, z_forward)
        first_y()
        x_forward(4)
        z_forward(3)
        first_z()
        spectral(derive_phase)
        loop(0, 3, send_derived)
        loop(1, 4, y_forward)
        spectral(derive_vortex)
        loop(3, 6, send_derived)
        z_forward(4)

        g0 = forward_count
        h0 = forward_count

        def phase_planes():
            col_arrived(g0)
            data = joined(g0)
            at_lane = lax.broadcasted_iota(jnp.int32, (1, row_lanes), 1)
            owner = at_lane // col_lanes
            lane_kx = owner * (kx_col - kx_own) + at_lane // rows_y + row_kx
            row_emit(h0, dot(zr_tab[...], data) * lane_kx.astype(f32))
            row = lax.broadcasted_iota(jnp.int32, (2 * modes_z, 1), 0)
            kz = jnp.where(row >= modes_z, row - modes_z, row) - half_z
            scaled = (data.astype(f32) * (kz.astype(f32) * (NX / total_z))).astype(bf16)
            row_emit(h0 + 1, dot(zr_tab[...], scaled))

        def to_field(i):
            derived[i] = x_inverse(h0 + i)

        def make_advect(at):
            lines[0, at, :] = (
                fields[1, at, :] * derived[0, at, :]
                + fields[2, at, :] * derived[2, at, :]
                + fields[3, at, :] * derived[1, at, :]
            ).astype(bf16)

        gradient_at = (0, 2, 1)
        vortex_at = (6, 5, 4)

        def make_forcing(which):
            def work(at):
                c = fields[0, at, :]
                potential = c * c * c - c - epsilon * epsilon * derived[3, at, :]
                for j in which:
                    p, q = (j + 1) % 3, (j + 2) % 3
                    lines[1 + j, at, :] = (
                        fields[1 + p, at, :] * derived[vortex_at[q], at, :]
                        - fields[1 + q, at, :] * derived[vortex_at[p], at, :]
                        + potential * derived[gradient_at[j], at, :]
                    ).astype(bf16)

            return work

        phase_planes()
        z_inverse(g0 + 1, h0 + 2)
        loop(0, 2, to_field)
        z_inverse(g0 + 2, h0 + 3)
        to_field(2)
        pointwise(make_advect)
        x_forward(5)
        z_inverse(g0 + 3, h0 + 4)
        to_field(3)
        z_forward(5)
        z_inverse(g0 + 4, h0 + 5)
        to_field(4)
        z_inverse(g0 + 5, h0 + 6)
        to_field(5)
        pointwise(make_forcing((0,)))
        x_forward(6)
        to_field(6)
        pointwise(make_forcing((1, 2)))
        loop(7, 9, x_forward)
        z_forward(6)
        loop(4, 6, y_forward)
        spectral(solve_phase)
        loop(7, 9, z_forward)
        loop(0, final_count, row_sent)
        loop(0, final_count, col_sent)
        thin_sent(0)
        wide_sent(0)
        y_inverse(0, 0)
        loop(6, 9, y_forward)
        spectral(solve_flow)
        last_z()
        def send_flow(e):
            y_inverse(e, e)

        loop(1, final_count, send_flow)
        last_y()

        z_inverse(0, 0)

        def finish(j):
            z_inverse(j + 1, j + 1)
            derived[j] = x_inverse(j)

        def emit(j):
            for z in range(planes):
                store(j, z).start()

        loop(0, 2, finish)
        emit(0)
        emit(1)
        derived[2] = x_inverse(2)
        emit(2)
        derived[3] = last_x()
        emit(3)
        loop(0, row_count, row_sent)
        loop(0, col_count, col_sent)
        thin_sent(0)
        wide_sent(0)
        for j in range(4):
            for z in range(planes):
                store(j, z).wait()

    sems = pltpu.SemaphoreType.DMA
    row_shape = (row_count, rows, 2 * planes, row_lanes)
    col_shape = (col_count, cols, 2 * modes_z, col_lanes)
    thin_shape = (1, rows, 2 * planes, wide_lanes)
    wide_shape = (1, cols, 2 * kx_col, points)
    scratch = []
    for shape in (row_shape, col_shape, thin_shape, wide_shape):
        scratch += [pltpu.VMEM(shape, bf16), pltpu.VMEM(shape, bf16)]
    scratch += [
        pltpu.VMEM((4, points, NX), f32),
        pltpu.VMEM((5, points, NX), bf16),
        pltpu.VMEM((derived_count, points, NX), f32),
        pltpu.VMEM((9, 2, own, KY), f32),
        pltpu.VMEM((derived_lines, 2 * own, KY), bf16),
    ]
    scratch += [pltpu.VMEM(t.shape, bf16) for t in made_tables]
    scratch += [pltpu.VMEM((2 * KC, NX), bf16), pltpu.VMEM((KY, 2 * NY), bf16)]
    for shape, size in ((row_shape, rows), (col_shape, cols), (thin_shape, rows), (wide_shape, cols)):
        scratch += [sems((shape[0], size - 1)), sems((shape[0], size - 1))]
    scratch += [sems((4, planes)), sems((len(made_tables),)), sems((4, planes))]
    hbm = pl.BlockSpec(memory_space=pltpu.HBM)
    out_shape = [
        jax.ShapeDtypeStruct(phase.shape, f32),
        jax.ShapeDtypeStruct(velocity.shape, f32),
    ]
    result = pl.pallas_call(
        body,
        in_specs=[hbm] * (2 + len(made_tables)),
        out_specs=[hbm, hbm],
        out_shape=out_shape,
        scratch_shapes=scratch,
        compiler_params=pltpu.CompilerParams(
            collective_id=0, has_side_effects=True, vmem_limit_bytes=67_043_328
        ),
        cost_estimate=pl.CostEstimate(
            flops=8_000_000_000, bytes_accessed=1 << 23, transcendentals=0
        ),
    )(phase, velocity, *made_tables)

    cuts = 4
    part = rows_y // cuts

    def deliver(phase_in, flow_in, phase_out, flow_out, held, load_sem, store_sem):
        def copies(j, k):
            at = pl.ds(k * part, part)
            source = phase_in.at[at] if j == 0 else flow_in.at[j - 1, at]
            target = phase_out.at[at] if j == 0 else flow_out.at[j - 1, at]
            load = pltpu.make_async_copy(source, held.at[j, at], load_sem.at[j, k])
            return load, pltpu.make_async_copy(held.at[j, at], target, store_sem.at[j, k])

        for j in range(4):
            for k in range(cuts):
                copies(j, k)[0].start()
        for j in range(4):
            for k in range(cuts):
                copies(j, k)[0].wait()
                copies(j, k)[1].start()
        for j in range(4):
            for k in range(cuts):
                copies(j, k)[1].wait()

    return tuple(
        pl.pallas_call(
            deliver,
            in_specs=[hbm, hbm],
            out_specs=[hbm, hbm],
            out_shape=out_shape,
            scratch_shapes=[
                pltpu.VMEM((4,) + phase.shape, f32), sems((4, cuts)), sems((4, cuts)),
            ],
            compiler_params=pltpu.CompilerParams(vmem_limit_bytes=67_043_328),
            cost_estimate=pl.CostEstimate(
                flops=1_000_000, bytes_accessed=1 << 23, transcendentals=0
            ),
        )(*result)
    )


def solution(mesh):
    cols, rows = mesh.shape["col"], mesh.shape["row"]

    def on_device(phase, velocity):
        rows_y, planes = phase.shape[0], phase.shape[1]
        kx_own = KC // (rows * cols)
        modes_z = 2 * (3 * planes * rows // 8)
        aligned = planes == 8 and 2 * rows_y == LANES and cols % 2 == 0
        exact = KC == kx_own * rows * cols and kx_own % 2 == 0 and modes_z % 8 == 0
        if aligned and exact:
            return fast_device((cols, rows, rows_y, planes), phase, velocity)
        return plain_device(phase, velocity)

    return jax.shard_map(
        on_device,
        mesh=mesh,
        in_specs=(P("col", "row", None), P(None, "col", "row", None)),
        out_specs=(P("col", "row", None), P(None, "col", "row", None)),
        check_vma=False,
    )
```

```python
import math

import jax
import jax.numpy as jnp
import ml_dtypes
import numpy as np
from jax import lax
from jax.experimental import pallas as pl
from jax.experimental.pallas import tpu as pltpu
from jax.sharding import PartitionSpec as P

NX = 512
NY = 512
KC = 192
KY = 384


time_step = 0.001
epsilon = 0.01
mobility = 1.0
reynolds = 100.0
stabilizer = 2.0


def cos_sin(row_index, col_index, period):
    residue = row_index[:, None] * col_index[None, :] % period
    angles = residue.astype(jnp.float32) * (2.0 * math.pi / period)
    return jnp.stack([jnp.cos(angles), jnp.sin(angles)]).astype(jnp.bfloat16)


def pair_sum(pieces, direction, stack_axis):
    if direction < 0:
        real_part = pieces[0, 0] + pieces[1, 1]
        imag_part = pieces[1, 0] - pieces[0, 1]
    else:
        real_part = pieces[0, 0] - pieces[1, 1]
        imag_part = pieces[0, 1] + pieces[1, 0]
    return jnp.stack([real_part, imag_part], axis=stack_axis)


def times_i(values):
    return jnp.stack([-values[:, 1], values[:, 0]], axis=1)


def phase_terms(phase, velocity, gradient, lap_field):
    advect = velocity[0] * gradient[0] + velocity[1] * gradient[1] + velocity[2] * gradient[2]
    bulk_term = phase * phase * phase - phase
    potential = bulk_term - epsilon * epsilon * lap_field
    return (advect, bulk_term, potential)


def momentum(velocity, vortex, gradient, potential):
    return jnp.stack(
        [
            velocity[1] * vortex[2] - velocity[2] * vortex[1] + potential * gradient[0],
            velocity[2] * vortex[0] - velocity[0] * vortex[2] + potential * gradient[1],
            velocity[0] * vortex[1] - velocity[1] * vortex[0] + potential * gradient[2],
        ]
    )


def plain_device(phase, velocity):
    col_count = lax.axis_size("col")
    row_count = lax.axis_size("row")
    rows_y = phase.shape[0]
    planes = phase.shape[1]
    total_z = planes * row_count
    half_z = 3 * total_z // 8
    modes_z = 2 * half_z
    kx_local = KC // col_count
    ky_local = KY // row_count
    scale_inv = 1.0 / (NX * NY * total_z)
    table_x = cos_sin(jnp.arange(NX, dtype=jnp.int32), jnp.arange(KC, dtype=jnp.int32), NX)
    table_y = cos_sin(jnp.arange(NY, dtype=jnp.int32), jnp.arange(KY, dtype=jnp.int32) - KC, NY)
    table_z = cos_sin(
        jnp.arange(total_z, dtype=jnp.int32), jnp.arange(modes_z, dtype=jnp.int32) - half_z, total_z
    )
    y_forward = table_y.reshape(2, col_count, rows_y, KY)
    y_inverse = table_y.reshape(2, col_count, rows_y, row_count, ky_local)
    z_table = table_z.reshape(2, row_count, planes, modes_z)
    weight = jnp.where(jnp.arange(KC) == 0, 1.0, 2.0).astype(jnp.bfloat16)[:, None, None, None]

    def along_y(incoming):
        field_count = incoming.shape[1]
        shaped = incoming.reshape(incoming.shape[0], field_count, col_count, 2, rows_y, planes)
        pieces = jnp.einsum(
            "afcpyz,tcyb->ptafbz", shaped, y_forward, preferred_element_type=jnp.float32
        )
        joined = pair_sum(pieces, -1, 2).astype(jnp.bfloat16)
        return joined.reshape(incoming.shape[0], field_count, 2, KY * planes)

    def along_z(incoming):
        field_count = incoming.shape[1]
        shaped = incoming.reshape(incoming.shape[0], field_count, 2, row_count, ky_local, planes)
        pieces = jnp.einsum(
            "afprbz,trzm->ptafbm", shaped, z_table, preferred_element_type=jnp.float32
        )
        joined = pair_sum(pieces, -1, 2) * scale_inv
        return joined.reshape(incoming.shape[0], field_count, 2, ky_local * modes_z)

    def back_y(incoming):
        field_count = incoming.shape[1]
        shaped = incoming.reshape(incoming.shape[0], field_count, 2, row_count, planes, ky_local)
        pieces = jnp.einsum(
            "afprzb,tcyrb->ptafcyz", shaped, y_inverse, preferred_element_type=jnp.float32
        )
        joined = pair_sum(pieces, 1, 3).astype(jnp.bfloat16)
        return joined.reshape(incoming.shape[0], field_count, col_count * 2 * rows_y * planes)

    def back_x(incoming):
        field_count = incoming.shape[1]
        shaped = incoming.reshape(KC, field_count, 2, rows_y, planes)
        scaled = jnp.stack([shaped[:, :, 0] * weight, -(shaped[:, :, 1] * weight)], axis=2)
        return jnp.einsum("afpyz,pxa->fyzx", scaled, table_x, preferred_element_type=jnp.float32)

    def forward(fields):
        field_count = fields.shape[0]
        pieces = jnp.einsum(
            "fyzx,txa->tafyz",
            fields.astype(jnp.bfloat16),
            table_x,
            preferred_element_type=jnp.float32,
        )
        x_lines = jnp.stack([pieces[0], -pieces[1]], axis=2).astype(jnp.bfloat16)
        x_lines = x_lines.reshape(KC, field_count, 2 * rows_y * planes)
        spread = along_y(lax.all_to_all(x_lines, "col", split_axis=0, concat_axis=2, tiled=True))
        return along_z(lax.all_to_all(spread, "row", split_axis=3, concat_axis=3, tiled=True))

    def inverse(spectra):
        field_count = spectra.shape[1]
        shaped = spectra.astype(jnp.bfloat16).reshape(kx_local, field_count, 2, ky_local, modes_z)
        pieces = jnp.einsum(
            "afpbm,trzm->ptafrzb", shaped, z_table, preferred_element_type=jnp.float32
        )
        z_planes = (
            pair_sum(pieces, 1, 2)
            .astype(jnp.bfloat16)
            .reshape(kx_local, field_count, 2, total_z * ky_local)
        )
        spread = back_y(lax.all_to_all(z_planes, "row", split_axis=3, concat_axis=3, tiled=True))
        return back_x(lax.all_to_all(spread, "col", split_axis=2, concat_axis=0, tiled=True))

    spectra = forward(jnp.concatenate([phase[None], velocity], axis=0))
    wave_x = (lax.axis_index("col") * kx_local + jnp.arange(kx_local, dtype=jnp.int32)).astype(
        jnp.float32
    )[:, None, None]
    modes_y = lax.axis_index("row") * ky_local + jnp.arange(ky_local, dtype=jnp.int32) - KC
    wave_y = jnp.broadcast_to(modes_y.astype(jnp.float32)[:, None], (ky_local, modes_z)).reshape(-1)
    z_values = (jnp.arange(modes_z, dtype=jnp.int32) - half_z).astype(jnp.float32) * (NX / total_z)
    wave_z = jnp.broadcast_to(z_values[None, :], (ky_local, modes_z)).reshape(-1)
    squared = wave_x * wave_x + wave_y * wave_y + wave_z * wave_z
    coeff_phase = spectra[:, 0]
    coeff_u = spectra[:, 1]
    coeff_v = spectra[:, 2]
    coeff_w = spectra[:, 3]
    gradients = [
        times_i(wave_x * coeff_phase),
        times_i(wave_y * coeff_phase),
        times_i(wave_z * coeff_phase),
    ]
    laplace = -squared * coeff_phase
    vortex_hat = [
        times_i(wave_y * coeff_w - wave_z * coeff_v),
        times_i(wave_z * coeff_u - wave_x * coeff_w),
        times_i(wave_x * coeff_v - wave_y * coeff_u),
    ]
    leading = inverse(jnp.stack(gradients + [laplace], axis=1))
    advect, bulk_term, potential = phase_terms(phase, velocity, leading[0:3], leading[3])
    phase_side = forward(jnp.stack([advect, bulk_term]))
    vortex = inverse(jnp.stack(vortex_hat, axis=1))
    flow_side = forward(momentum(velocity, vortex, leading[0:3], potential))
    nonlinear = jnp.concatenate([phase_side, flow_side], axis=1)
    mean_mode = (wave_x == 0) & (wave_y == 0) & (wave_z == 0)
    advect_hat = jnp.where(mean_mode, 0.0, nonlinear[:, 0])
    bulk_hat = nonlinear[:, 1]
    stable_part = 1.0 / time_step + mobility * stabilizer * squared
    new_phase = (stable_part * coeff_phase - advect_hat - mobility * squared * bulk_hat) / (
        stable_part + mobility * epsilon * epsilon * squared * squared
    )
    viscous = 1.0 / time_step + squared / reynolds
    unprojected = [
        (spectra[:, 1 + j] / time_step + nonlinear[:, 2 + j]) / viscous for j in range(3)
    ]
    normal_part = (
        wave_x * unprojected[0] + wave_y * unprojected[1] + wave_z * unprojected[2]
    ) / jnp.maximum(squared, 1.0)
    waves = [wave_x, wave_y, wave_z]
    new_flow = [unprojected[j] - waves[j] * normal_part for j in range(3)]
    result = inverse(jnp.stack([new_phase] + new_flow, axis=1))
    return (result[0], result[1:4])


def tables(cols, rows, rows_y, planes):
    total_z = planes * rows
    half_z = 3 * total_z // 8
    modes_z = 2 * half_z
    kx_row = KC // rows

    def pair(first, second, period):
        residue = first[:, None] * second[None, :] % period
        angles = residue.astype(np.float32) * np.float32(2.0 * math.pi / period)
        return [np.cos(angles).astype(ml_dtypes.bfloat16), np.sin(angles).astype(ml_dtypes.bfloat16)]

    cos_x, sin_x = pair(np.arange(KC), np.arange(NX), NX)
    cos_y, sin_y = pair(np.arange(NY), np.arange(KY) - KC, NY)
    cos_z, sin_z = pair(np.arange(total_z), np.arange(modes_z) - half_z, total_z)
    order = np.arange(KC).reshape(cols, rows, kx_row // cols).transpose(1, 0, 2).reshape(KC)
    x_table = np.stack([cos_x[order], -sin_x[order]]).reshape(2, rows, kx_row // 2, 2, NX)
    x_table = x_table.transpose(1, 0, 3, 2, 4).reshape(2 * KC, NX)
    y_forward = np.concatenate([cos_y, sin_y], axis=1)
    cz, sz = (t.reshape(rows, planes, modes_z) for t in (cos_z, sin_z))
    z_forward = np.stack([np.stack([cz, sz], 1), np.stack([-sz, cz], 1)])
    z_forward = z_forward.transpose(0, 4, 1, 2, 3).reshape(2 * modes_z, 2 * total_z)
    z_inverse = np.stack([np.stack([cz, -sz], 2), np.stack([sz, cz], 2)], 1)
    z_inverse = z_inverse.reshape(2 * total_z, 2 * modes_z)
    z_rotated = np.concatenate([z_inverse[:, modes_z:], -z_inverse[:, :modes_z]], axis=1)
    x_wide = np.stack([cos_x, -sin_x]).reshape(2, cols, kx_row * rows // cols, NX)
    x_wide = x_wide.transpose(1, 0, 2, 3).reshape(2 * KC, NX)
    made = (x_wide, y_forward, z_forward, z_inverse, z_rotated, x_table)
    return [jnp.asarray(t.astype(ml_dtypes.bfloat16)) for t in made]


def dot(first, second, dims=((1,), (0,))):
    return lax.dot_general(first, second, (dims, ((), ())), preferred_element_type=jnp.float32)


LANES = 128


def fast_device(sizes, phase, velocity):
    cols, rows, rows_y, planes = sizes
    total_z = planes * rows
    half_z = 3 * total_z // 8
    modes_z = 2 * half_z
    kx_row = KC // rows
    kx_own = kx_row // cols
    pairs = kx_row // 2
    points = rows_y * planes
    row_lanes = kx_row * rows_y
    col_lanes = kx_own * rows_y
    own = kx_own * modes_z
    scale_inv = 1.0 / (NX * NY * total_z)
    made_tables = tables(cols, rows, rows_y, planes)
    f32, bf16 = jnp.float32, jnp.bfloat16
    forward_count, derived_count, derived_lines, final_count = 7, 7, 6, 3
    row_count = forward_count + derived_count
    col_count = forward_count + derived_lines
    kx_col = kx_own * rows
    wide_lanes = kx_own * KY

    def partner(me, d, size):
        if size & (size - 1):
            return lax.rem(me + d, size)
        peer, bit = 0, 1
        while bit < size:
            mine = (me // bit) % 2
            peer = peer + bit * (1 - mine if d & bit else mine)
            bit *= 2
        return peer

    def exchange(axis, size, src, dst, send, recv):
        me = lax.axis_index(axis)

        def copy(f, d):
            peer = partner(me, d, size)
            return pltpu.make_async_remote_copy(
                src_ref=src.at[f, peer],
                dst_ref=dst.at[f, me],
                send_sem=send.at[f, d - 1],
                recv_sem=recv.at[f, d - 1],
                device_id={axis: peer},
                device_id_type=pl.DeviceIdType.MESH,
            )

        def start(f):
            for d in reversed(range(1, size)):
                copy(f, d).start()
            dst[f, me] = src[f, me]

        def arrived(f):
            for d in range(1, size):
                copy(f, d).wait_recv()

        def sent(f):
            for d in range(1, size):
                copy(f, d).wait_send()

        return start, arrived, sent

    def greet():
        barrier = pltpu.get_barrier_semaphore()
        for axis, size in (("col", cols), ("row", rows)):
            for d in range(1, size):
                peer = lax.rem(lax.axis_index(axis) + d, size)
                pl.semaphore_signal(
                    barrier, inc=1, device_id={axis: peer}, device_id_type=pl.DeviceIdType.MESH
                )

    def greeted():
        pl.semaphore_wait(pltpu.get_barrier_semaphore(), cols + rows - 2)

    def swap_halves(first, second):
        half = LANES // 2
        low = jnp.concatenate([first[:, :half], second[:, :half]], axis=1)
        high = jnp.concatenate([first[:, half:], second[:, half:]], axis=1)
        return low, high

    def body(*refs):
        phase_in, flow_in = refs[:2]
        table_in = refs[2:8]
        phase_out, flow_out = refs[8:10]
        (
            row_src, row_dst, col_src, col_dst, thin_src, thin_dst, wide_src, wide_dst,
            fields, lines, derived, coeff, ready,
            xw_tab, yf_tab, zf_tab, zi_tab, zr_tab, x_tab, yi_tab,
            row_send, row_recv, col_send, col_recv, thin_send, thin_recv, wide_send, wide_recv,
            load_sem, table_sem, store_sem,
        ) = refs[10:]
        table_refs = (xw_tab, yf_tab, zf_tab, zi_tab, zr_tab, x_tab)
        row_start, row_arrived, row_sent = exchange("row", rows, row_src, row_dst, row_send, row_recv)
        col_start, col_arrived, col_sent = exchange("col", cols, col_src, col_dst, col_send, col_recv)
        thin_start, thin_arrived, thin_sent = exchange(
            "row", rows, thin_src, thin_dst, thin_send, thin_recv
        )
        wide_start, wide_arrived, wide_sent = exchange(
            "col", cols, wide_src, wide_dst, wide_send, wide_recv
        )

        def load(j, z):
            source = phase_in.at[:, z, :] if j == 0 else flow_in.at[j - 1, :, z, :]
            target = fields.at[j, pl.ds(z * rows_y, rows_y), :]
            return pltpu.make_async_copy(source, target, load_sem.at[j, z])

        def store(j, z):
            target = phase_out.at[:, z, :] if j == 0 else flow_out.at[j - 1, :, z, :]
            source = derived.at[j, pl.ds(z * rows_y, rows_y), :]
            return pltpu.make_async_copy(source, target, store_sem.at[j, z])

        def table_copy(k):
            return pltpu.make_async_copy(table_in[k], table_refs[k], table_sem.at[k])

        row_kx = lax.axis_index("row") * kx_own
        own_kx = lax.axis_index("col") * kx_col + row_kx

        def x_forward(f):
            made = dot(x_tab[...], lines[lax.rem(f, 5)], ((1,), (1,)))
            for r in range(rows):
                parts = []
                for p in range(2):
                    base = (r * 2 + p) * kx_row
                    even = made[base : base + pairs]
                    odd = made[base + pairs : base + kx_row]
                    planes_made = []
                    for j in range(planes // 2):
                        at = slice(j * LANES, (j + 1) * LANES)
                        planes_made.extend(swap_halves(even[:, at], odd[:, at]))
                    parts.append(jnp.swapaxes(jnp.stack(planes_made), 0, 1))
                both = jnp.concatenate(parts, axis=1).astype(bf16)
                for k in range(pairs):
                    row_src[f - 1, r, :, k * LANES : (k + 1) * LANES] = both[k]
            row_start(f - 1)

        def x_inverse(h):
            row_arrived(h)
            made = []
            for r in range(rows):
                whole_lines = row_dst[h, r].astype(f32)
                tiles = jnp.stack([whole_lines[:, k * LANES : (k + 1) * LANES] for k in range(pairs)])
                for p in range(2):
                    by_plane = jnp.swapaxes(tiles[:, p * planes : (p + 1) * planes], 0, 1)
                    even, odd = [], []
                    for j in range(planes // 2):
                        low, high = swap_halves(by_plane[2 * j], by_plane[2 * j + 1])
                        even.append(low)
                        odd.append(high)
                    made.append(jnp.concatenate(even, axis=1))
                    made.append(jnp.concatenate(odd, axis=1))
            gathered = jnp.concatenate(made, axis=0).astype(bf16)
            return dot(gathered, x_tab[...], ((0,), (0,)))

        def z_forward(f):
            row_arrived(f - 1)
            stacked = row_dst[f - 1].reshape(2 * total_z, row_lanes)
            made = dot(zf_tab[...], stacked).astype(bf16)
            for c in range(cols):
                col_src[f - 1, c] = made[:, c * col_lanes : (c + 1) * col_lanes]
            col_start(f - 1)

        def joined(g):
            return jnp.concatenate([col_dst[g, c] for c in range(cols)], axis=1)

        def row_emit(h, made):
            made = made.astype(bf16)
            for r in range(rows):
                row_src[h, r] = made[r * 2 * planes : (r + 1) * 2 * planes]
            row_start(h)

        def inverse_table():
            for t in range(2):
                part = yf_tab[:, t * KY : (t + 1) * KY].astype(f32)
                yi_tab[:, t * NY : (t + 1) * NY] = part.T.astype(bf16)

        def wide_x(slot, line):
            made = dot(xw_tab[...], lines[line], ((1,), (1,))).astype(bf16)
            wide_src[slot] = made.reshape(cols, 2 * kx_col, points)

        def wide_y(slot):
            wide_arrived(slot)
            lhs = jnp.concatenate(
                [
                    jnp.concatenate(
                        [wide_dst[slot, c, :, z * rows_y : (z + 1) * rows_y] for c in range(cols)],
                        axis=1,
                    )
                    for z in range(planes)
                ],
                axis=0,
            )
            made = dot(lhs, yf_tab[...]).reshape(planes, 2 * kx_col, 2 * KY)
            first, second = made[:, :kx_col], made[:, kx_col:]
            real = jnp.swapaxes(first[:, :, :KY] + second[:, :, KY:], 0, 1)
            imag = jnp.swapaxes(second[:, :, :KY] - first[:, :, KY:], 0, 1)
            both = jnp.concatenate([real, imag], axis=1).astype(bf16)
            for k in range(kx_col):
                r, a = k // kx_own, k % kx_own
                thin_src[slot, r, :, a * KY : (a + 1) * KY] = both[k]
            thin_start(slot)

        def wide_z(slot, f):
            thin_arrived(slot)
            stacked = thin_dst[slot].reshape(2 * total_z, wide_lanes)
            made = dot(zf_tab[...], stacked) * scale_inv
            for p in range(2):
                for a in range(kx_own):
                    coeff[f, p, a * modes_z : (a + 1) * modes_z, :] = made[
                        p * modes_z : (p + 1) * modes_z, a * KY : (a + 1) * KY
                    ]

        def last_z():
            parts = []
            for p in range(2):
                parts.append(
                    jnp.concatenate(
                        [coeff[0, p, a * modes_z : (a + 1) * modes_z, :] for a in range(kx_own)], axis=1
                    )
                )
            made = dot(zi_tab[...], jnp.concatenate(parts, axis=0).astype(bf16)).astype(bf16)
            for r in range(rows):
                thin_src[0, r] = made[r * 2 * planes : (r + 1) * 2 * planes]
            thin_start(0)

        def last_y():
            thin_arrived(0)
            lhs = jnp.concatenate(
                [
                    thin_dst[0, r, :, a * KY : (a + 1) * KY]
                    for r in range(rows)
                    for a in range(kx_own)
                ],
                axis=0,
            )
            made = dot(lhs, yi_tab[...]).reshape(kx_col, 2 * planes, 2 * NY)
            first, second = made[:, :planes], made[:, planes:]
            real = jnp.swapaxes(first[:, :, :NY] - second[:, :, NY:], 0, 1)
            imag = jnp.swapaxes(first[:, :, NY:] + second[:, :, :NY], 0, 1)
            both = jnp.concatenate([real, imag], axis=1).astype(bf16)
            for c in range(cols):
                wide_src[0, c] = jnp.concatenate(
                    [both[z, :, c * rows_y : (c + 1) * rows_y] for z in range(planes)], axis=1
                )
            wide_start(0)

        def last_x():
            wide_arrived(0)
            gathered = wide_dst[0].reshape(2 * KC, points)
            return dot(gathered, xw_tab[...], ((0,), (0,)))

        def z_inverse(g, h):
            col_arrived(g)
            row_emit(h, dot(zi_tab[...], joined(g)))

        def y_forward(f):
            col_arrived(f - 1)
            lhs = jnp.concatenate(
                [
                    jnp.concatenate(
                        [col_dst[f - 1, c, :, a * rows_y : (a + 1) * rows_y] for c in range(cols)], axis=1
                    )
                    for a in range(kx_own)
                ],
                axis=0,
            )
            made = dot(lhs, yf_tab[...]).reshape(kx_own, 2 * modes_z, 2 * KY)
            first, second = made[:, :modes_z], made[:, modes_z:]
            real = first[:, :, :KY] + second[:, :, KY:]
            imag = second[:, :, :KY] - first[:, :, KY:]
            coeff[f, 0] = real.reshape(own, KY) * scale_inv
            coeff[f, 1] = imag.reshape(own, KY) * scale_inv

        def y_inverse(e, g):
            made = dot(ready[e], yi_tab[...])
            first, second = made[:own], made[own:]
            real = (first[:, :NY] - second[:, NY:]).reshape(kx_own, modes_z, NY)
            imag = (first[:, NY:] + second[:, :NY]).reshape(kx_own, modes_z, NY)
            both = jnp.concatenate([real, imag], axis=1).astype(bf16)
            for c in range(cols):
                col_src[g, c] = jnp.concatenate(
                    [both[a, :, c * rows_y : (c + 1) * rows_y] for a in range(kx_own)], axis=1
                )
            col_start(g)

        block = 2 * modes_z

        def spectral(work):
            def step(i, carry):
                base = pl.multiple_of(i * block, block)
                at = pl.ds(base, block)
                row = lax.broadcasted_iota(jnp.int32, (block, KY), 0)
                upper = row >= modes_z
                kx = own_kx + 2 * i + jnp.where(upper, 1, 0)
                kz = jnp.where(upper, row - modes_z, row) - half_z
                ky = lax.broadcasted_iota(jnp.int32, (block, KY), 1) - KC
                weight = jnp.where(kx == 0, 1.0, 2.0)
                mean_mode = (kx == 0) & (ky == 0) & (kz == 0)
                wx, wy = kx.astype(f32), ky.astype(f32)
                wz = kz.astype(f32) * (NX / total_z)
                k2 = wx * wx + wy * wy + wz * wz

                def get(f):
                    return coeff[f, 0, at, :], coeff[f, 1, at, :]

                def put(e, real, imag):
                    if e is None:
                        coeff[0, 0, at, :] = real * weight
                        coeff[0, 1, at, :] = imag * weight
                        return
                    ready[e, at, :] = (real * weight).astype(bf16)
                    ready[e, pl.ds(pl.multiple_of(own + base, block), block), :] = (
                        imag * weight
                    ).astype(bf16)

                work(get, put, wx, wy, wz, k2, mean_mode)
                return carry

            lax.fori_loop(0, own // block, step, 0)

        def derive_phase(get, put, wx, wy, wz, k2, mean_mode):
            real, imag = get(0)
            put(0, real, imag)
            put(1, -(wy * imag), wy * real)
            put(2, -k2 * real, -k2 * imag)

        def derive_vortex(get, put, wx, wy, wz, k2, mean_mode):
            w = [wx, wy, wz]
            got = [get(1 + j) for j in range(3)]
            for e, j in ((3, 2), (4, 1), (5, 0)):
                p, q = (j + 1) % 3, (j + 2) % 3
                real = -(w[p] * got[q][1] - w[q] * got[p][1])
                put(e, real, w[p] * got[q][0] - w[q] * got[p][0])

        def solve_phase(get, put, wx, wy, wz, k2, mean_mode):
            old, bulk_hat, advect_hat = get(0), get(4), get(5)
            stable = 1.0 / time_step + mobility * stabilizer * k2
            below = stable + mobility * epsilon * epsilon * k2 * k2
            made = []
            for p in range(2):
                kept = jnp.where(mean_mode, 0.0, advect_hat[p])
                made.append((stable * old[p] - kept - mobility * k2 * bulk_hat[p]) / below)
            put(0, made[0], made[1])

        forcing_slot = (8, 6, 7)

        def solve_flow(get, put, wx, wy, wz, k2, mean_mode):
            viscous = 1.0 / time_step + k2 / reynolds
            largest = jnp.maximum(k2, 1.0)
            w = [wx, wy, wz]
            old = [get(1 + j) for j in range(3)]
            added = [get(forcing_slot[j]) for j in range(3)]
            made = [[], [], []]
            for p in range(2):
                free = [(old[j][p] / time_step + added[j][p]) / viscous for j in range(3)]
                normal = (wx * free[0] + wy * free[1] + wz * free[2]) / largest
                for j in range(3):
                    made[j].append(free[j] - w[j] * normal)
            for j in range(3):
                put(1 + j if j < 2 else None, made[j][0], made[j][1])

        cut = 32

        def pointwise(work):
            def step(i, carry):
                work(pl.ds(pl.multiple_of(i * cut, cut), cut))
                return carry

            lax.fori_loop(0, points // cut, step, 0)

        def loop(begin, end, work):
            def step(i, carry):
                work(i)
                return carry

            lax.fori_loop(begin, end, step, 0)

        for z in range(planes):
            load(0, z).start()
        for k in range(len(table_refs)):
            table_copy(k).start()
        for j in range(1, 4):
            for z in range(planes):
                load(j, z).start()
        greet()

        def cast(f):
            def work(at):
                lines[f, at, :] = fields[f, at, :].astype(bf16)

            pointwise(work)

        def bring(f):
            for z in range(planes):
                load(f, z).wait()
            cast(f)

        def make_bulk(at):
            c = fields[0, at, :]
            lines[4, at, :] = (c * c * c - c).astype(bf16)

        def send_derived(e):
            y_inverse(e, forward_count + e)

        table_copy(0).wait()
        bring(0)
        wide_x(0, 0)
        greeted()
        wide_start(0)
        for k in range(1, len(table_refs)):
            table_copy(k).wait()
        for j in range(1, 4):
            bring(j)
        loop(1, 4, x_forward)
        inverse_table()
        pointwise(make_bulk)
        loop(1, 3, z_forward)
        wide_y(0)
        x_forward(4)
        z_forward(3)
        wide_z(0, 0)
        spectral(derive_phase)
        send_derived(0)
        loop(1, 3, y_forward)
        send_derived(1)
        y_forward(3)
        spectral(derive_vortex)
        loop(2, 6, send_derived)

        g0 = forward_count
        h0 = forward_count

        def phase_planes():
            col_arrived(g0)
            data = joined(g0)
            at_lane = lax.broadcasted_iota(jnp.int32, (1, row_lanes), 1)
            owner = at_lane // col_lanes
            lane_kx = owner * (kx_col - kx_own) + at_lane // rows_y + row_kx
            row_emit(h0, dot(zr_tab[...], data) * lane_kx.astype(f32))
            row = lax.broadcasted_iota(jnp.int32, (2 * modes_z, 1), 0)
            kz = jnp.where(row >= modes_z, row - modes_z, row) - half_z
            scaled = (data.astype(f32) * (kz.astype(f32) * (NX / total_z))).astype(bf16)
            row_emit(h0 + 1, dot(zr_tab[...], scaled))

        def to_field(i):
            derived[i] = x_inverse(h0 + i)

        def make_advect(at):
            lines[0, at, :] = (
                fields[1, at, :] * derived[0, at, :]
                + fields[2, at, :] * derived[2, at, :]
                + fields[3, at, :] * derived[1, at, :]
            ).astype(bf16)

        gradient_at = (0, 2, 1)
        vortex_at = (6, 5, 4)

        def make_forcing(which):
            def work(at):
                c = fields[0, at, :]
                potential = c * c * c - c - epsilon * epsilon * derived[3, at, :]
                for j in which:
                    p, q = (j + 1) % 3, (j + 2) % 3
                    lines[(3, 1, 2)[j], at, :] = (
                        fields[1 + p, at, :] * derived[vortex_at[q], at, :]
                        - fields[1 + q, at, :] * derived[vortex_at[p], at, :]
                        + potential * derived[gradient_at[j], at, :]
                    ).astype(bf16)

            return work

        phase_planes()
        z_inverse(g0 + 1, h0 + 2)
        loop(0, 2, to_field)
        z_inverse(g0 + 2, h0 + 3)
        to_field(2)
        pointwise(make_advect)
        x_forward(5)
        z_inverse(g0 + 3, h0 + 4)
        to_field(3)
        z_forward(4)
        z_forward(5)
        z_inverse(g0 + 4, h0 + 5)
        to_field(4)
        z_inverse(g0 + 5, h0 + 6)
        to_field(5)
        pointwise(make_forcing((0,)))
        wide_x(1, 3)
        wide_start(1)
        to_field(6)
        pointwise(make_forcing((1, 2)))
        loop(6, 8, x_forward)
        loop(4, 6, y_forward)
        spectral(solve_phase)
        loop(6, 8, z_forward)
        loop(0, final_count, row_sent)
        loop(0, final_count, col_sent)
        thin_sent(0)
        wide_sent(0)
        y_inverse(0, 0)
        wide_y(1)
        wide_z(1, 8)
        loop(6, 8, y_forward)
        spectral(solve_flow)
        last_z()
        def send_flow(e):
            y_inverse(e, e)

        loop(1, final_count, send_flow)
        last_y()

        z_inverse(0, 0)

        def finish(j):
            z_inverse(j + 1, j + 1)
            derived[j] = x_inverse(j)

        def emit(j):
            for z in range(planes):
                store(j, z).start()

        loop(0, 2, finish)
        emit(0)
        emit(1)
        derived[2] = x_inverse(2)
        emit(2)
        derived[3] = last_x()
        emit(3)
        loop(0, row_count, row_sent)
        loop(0, col_count, col_sent)
        loop(0, 2, thin_sent)
        loop(0, 2, wide_sent)
        for j in range(4):
            for z in range(planes):
                store(j, z).wait()

    sems = pltpu.SemaphoreType.DMA
    row_shape = (row_count, rows, 2 * planes, row_lanes)
    col_shape = (col_count, cols, 2 * modes_z, col_lanes)
    thin_shape = (2, rows, 2 * planes, wide_lanes)
    wide_shape = (2, cols, 2 * kx_col, points)
    scratch = []
    for shape in (row_shape, col_shape, thin_shape, wide_shape):
        scratch += [pltpu.VMEM(shape, bf16), pltpu.VMEM(shape, bf16)]
    scratch += [
        pltpu.VMEM((4, points, NX), f32),
        pltpu.VMEM((5, points, NX), bf16),
        pltpu.VMEM((derived_count, points, NX), f32),
        pltpu.VMEM((9, 2, own, KY), f32),
        pltpu.VMEM((derived_lines, 2 * own, KY), bf16),
    ]
    scratch += [pltpu.VMEM(t.shape, bf16) for t in made_tables]
    scratch += [pltpu.VMEM((KY, 2 * NY), bf16)]
    for shape, size in ((row_shape, rows), (col_shape, cols), (thin_shape, rows), (wide_shape, cols)):
        scratch += [sems((shape[0], size - 1)), sems((shape[0], size - 1))]
    scratch += [sems((4, planes)), sems((len(made_tables),)), sems((4, planes))]
    hbm = pl.BlockSpec(memory_space=pltpu.HBM)
    out_shape = [
        jax.ShapeDtypeStruct(phase.shape, f32),
        jax.ShapeDtypeStruct(velocity.shape, f32),
    ]
    result = pl.pallas_call(
        body,
        in_specs=[hbm] * (2 + len(made_tables)),
        out_specs=[hbm, hbm],
        out_shape=out_shape,
        scratch_shapes=scratch,
        compiler_params=pltpu.CompilerParams(
            collective_id=0, has_side_effects=True, vmem_limit_bytes=67_043_328
        ),
        cost_estimate=pl.CostEstimate(
            flops=8_000_000_000, bytes_accessed=1 << 23, transcendentals=0
        ),
    )(phase, velocity, *made_tables)

    cuts = 4
    part = rows_y // cuts

    def deliver(phase_in, flow_in, phase_out, flow_out, held, load_sem, store_sem):
        def copies(j, k):
            at = pl.ds(k * part, part)
            source = phase_in.at[at] if j == 0 else flow_in.at[j - 1, at]
            target = phase_out.at[at] if j == 0 else flow_out.at[j - 1, at]
            load = pltpu.make_async_copy(source, held.at[j, at], load_sem.at[j, k])
            return load, pltpu.make_async_copy(held.at[j, at], target, store_sem.at[j, k])

        for j in range(4):
            for k in range(cuts):
                copies(j, k)[0].start()
        for j in range(4):
            for k in range(cuts):
                copies(j, k)[0].wait()
                copies(j, k)[1].start()
        for j in range(4):
            for k in range(cuts):
                copies(j, k)[1].wait()

    return tuple(
        pl.pallas_call(
            deliver,
            in_specs=[hbm, hbm],
            out_specs=[hbm, hbm],
            out_shape=out_shape,
            scratch_shapes=[
                pltpu.VMEM((4,) + phase.shape, f32), sems((4, cuts)), sems((4, cuts)),
            ],
            compiler_params=pltpu.CompilerParams(vmem_limit_bytes=67_043_328),
            cost_estimate=pl.CostEstimate(
                flops=1_000_000, bytes_accessed=1 << 23, transcendentals=0
            ),
        )(*result)
    )


def solution(mesh):
    cols, rows = mesh.shape["col"], mesh.shape["row"]

    def on_device(phase, velocity):
        rows_y, planes = phase.shape[0], phase.shape[1]
        kx_own = KC // (rows * cols)
        modes_z = 2 * (3 * planes * rows // 8)
        aligned = planes == 8 and 2 * rows_y == LANES and cols % 2 == 0
        exact = KC == kx_own * rows * cols and kx_own % 2 == 0 and modes_z % 8 == 0
        if aligned and exact:
            return fast_device((cols, rows, rows_y, planes), phase, velocity)
        return plain_device(phase, velocity)

    return jax.shard_map(
        on_device,
        mesh=mesh,
        in_specs=(P("col", "row", None), P(None, "col", "row", None)),
        out_specs=(P("col", "row", None), P(None, "col", "row", None)),
        check_vma=False,
    )
```

```python
import math

import jax
import jax.numpy as jnp
import ml_dtypes
import numpy as np
from jax import lax
from jax.experimental import pallas as pl
from jax.experimental.pallas import tpu as pltpu
from jax.sharding import PartitionSpec as P

NX = 512
NY = 512
KC = 192
KY = 384


time_step = 0.001
epsilon = 0.01
mobility = 1.0
reynolds = 100.0
stabilizer = 2.0


def cos_sin(row_index, col_index, period):
    residue = row_index[:, None] * col_index[None, :] % period
    angles = residue.astype(jnp.float32) * (2.0 * math.pi / period)
    return jnp.stack([jnp.cos(angles), jnp.sin(angles)]).astype(jnp.bfloat16)


def pair_sum(pieces, direction, stack_axis):
    if direction < 0:
        real_part = pieces[0, 0] + pieces[1, 1]
        imag_part = pieces[1, 0] - pieces[0, 1]
    else:
        real_part = pieces[0, 0] - pieces[1, 1]
        imag_part = pieces[0, 1] + pieces[1, 0]
    return jnp.stack([real_part, imag_part], axis=stack_axis)


def times_i(values):
    return jnp.stack([-values[:, 1], values[:, 0]], axis=1)


def phase_terms(phase, velocity, gradient, lap_field):
    advect = velocity[0] * gradient[0] + velocity[1] * gradient[1] + velocity[2] * gradient[2]
    bulk_term = phase * phase * phase - phase
    potential = bulk_term - epsilon * epsilon * lap_field
    return (advect, bulk_term, potential)


def momentum(velocity, vortex, gradient, potential):
    return jnp.stack(
        [
            velocity[1] * vortex[2] - velocity[2] * vortex[1] + potential * gradient[0],
            velocity[2] * vortex[0] - velocity[0] * vortex[2] + potential * gradient[1],
            velocity[0] * vortex[1] - velocity[1] * vortex[0] + potential * gradient[2],
        ]
    )


def plain_device(phase, velocity):
    col_count = lax.axis_size("col")
    row_count = lax.axis_size("row")
    rows_y = phase.shape[0]
    planes = phase.shape[1]
    total_z = planes * row_count
    half_z = 3 * total_z // 8
    modes_z = 2 * half_z
    kx_local = KC // col_count
    ky_local = KY // row_count
    scale_inv = 1.0 / (NX * NY * total_z)
    table_x = cos_sin(jnp.arange(NX, dtype=jnp.int32), jnp.arange(KC, dtype=jnp.int32), NX)
    table_y = cos_sin(jnp.arange(NY, dtype=jnp.int32), jnp.arange(KY, dtype=jnp.int32) - KC, NY)
    table_z = cos_sin(
        jnp.arange(total_z, dtype=jnp.int32), jnp.arange(modes_z, dtype=jnp.int32) - half_z, total_z
    )
    y_forward = table_y.reshape(2, col_count, rows_y, KY)
    y_inverse = table_y.reshape(2, col_count, rows_y, row_count, ky_local)
    z_table = table_z.reshape(2, row_count, planes, modes_z)
    weight = jnp.where(jnp.arange(KC) == 0, 1.0, 2.0).astype(jnp.bfloat16)[:, None, None, None]

    def along_y(incoming):
        field_count = incoming.shape[1]
        shaped = incoming.reshape(incoming.shape[0], field_count, col_count, 2, rows_y, planes)
        pieces = jnp.einsum(
            "afcpyz,tcyb->ptafbz", shaped, y_forward, preferred_element_type=jnp.float32
        )
        joined = pair_sum(pieces, -1, 2).astype(jnp.bfloat16)
        return joined.reshape(incoming.shape[0], field_count, 2, KY * planes)

    def along_z(incoming):
        field_count = incoming.shape[1]
        shaped = incoming.reshape(incoming.shape[0], field_count, 2, row_count, ky_local, planes)
        pieces = jnp.einsum(
            "afprbz,trzm->ptafbm", shaped, z_table, preferred_element_type=jnp.float32
        )
        joined = pair_sum(pieces, -1, 2) * scale_inv
        return joined.reshape(incoming.shape[0], field_count, 2, ky_local * modes_z)

    def back_y(incoming):
        field_count = incoming.shape[1]
        shaped = incoming.reshape(incoming.shape[0], field_count, 2, row_count, planes, ky_local)
        pieces = jnp.einsum(
            "afprzb,tcyrb->ptafcyz", shaped, y_inverse, preferred_element_type=jnp.float32
        )
        joined = pair_sum(pieces, 1, 3).astype(jnp.bfloat16)
        return joined.reshape(incoming.shape[0], field_count, col_count * 2 * rows_y * planes)

    def back_x(incoming):
        field_count = incoming.shape[1]
        shaped = incoming.reshape(KC, field_count, 2, rows_y, planes)
        scaled = jnp.stack([shaped[:, :, 0] * weight, -(shaped[:, :, 1] * weight)], axis=2)
        return jnp.einsum("afpyz,pxa->fyzx", scaled, table_x, preferred_element_type=jnp.float32)

    def forward(fields):
        field_count = fields.shape[0]
        pieces = jnp.einsum(
            "fyzx,txa->tafyz",
            fields.astype(jnp.bfloat16),
            table_x,
            preferred_element_type=jnp.float32,
        )
        x_lines = jnp.stack([pieces[0], -pieces[1]], axis=2).astype(jnp.bfloat16)
        x_lines = x_lines.reshape(KC, field_count, 2 * rows_y * planes)
        spread = along_y(lax.all_to_all(x_lines, "col", split_axis=0, concat_axis=2, tiled=True))
        return along_z(lax.all_to_all(spread, "row", split_axis=3, concat_axis=3, tiled=True))

    def inverse(spectra):
        field_count = spectra.shape[1]
        shaped = spectra.astype(jnp.bfloat16).reshape(kx_local, field_count, 2, ky_local, modes_z)
        pieces = jnp.einsum(
            "afpbm,trzm->ptafrzb", shaped, z_table, preferred_element_type=jnp.float32
        )
        z_planes = (
            pair_sum(pieces, 1, 2)
            .astype(jnp.bfloat16)
            .reshape(kx_local, field_count, 2, total_z * ky_local)
        )
        spread = back_y(lax.all_to_all(z_planes, "row", split_axis=3, concat_axis=3, tiled=True))
        return back_x(lax.all_to_all(spread, "col", split_axis=2, concat_axis=0, tiled=True))

    spectra = forward(jnp.concatenate([phase[None], velocity], axis=0))
    wave_x = (lax.axis_index("col") * kx_local + jnp.arange(kx_local, dtype=jnp.int32)).astype(
        jnp.float32
    )[:, None, None]
    modes_y = lax.axis_index("row") * ky_local + jnp.arange(ky_local, dtype=jnp.int32) - KC
    wave_y = jnp.broadcast_to(modes_y.astype(jnp.float32)[:, None], (ky_local, modes_z)).reshape(-1)
    z_values = (jnp.arange(modes_z, dtype=jnp.int32) - half_z).astype(jnp.float32) * (NX / total_z)
    wave_z = jnp.broadcast_to(z_values[None, :], (ky_local, modes_z)).reshape(-1)
    squared = wave_x * wave_x + wave_y * wave_y + wave_z * wave_z
    coeff_phase = spectra[:, 0]
    coeff_u = spectra[:, 1]
    coeff_v = spectra[:, 2]
    coeff_w = spectra[:, 3]
    gradients = [
        times_i(wave_x * coeff_phase),
        times_i(wave_y * coeff_phase),
        times_i(wave_z * coeff_phase),
    ]
    laplace = -squared * coeff_phase
    vortex_hat = [
        times_i(wave_y * coeff_w - wave_z * coeff_v),
        times_i(wave_z * coeff_u - wave_x * coeff_w),
        times_i(wave_x * coeff_v - wave_y * coeff_u),
    ]
    leading = inverse(jnp.stack(gradients + [laplace], axis=1))
    advect, bulk_term, potential = phase_terms(phase, velocity, leading[0:3], leading[3])
    phase_side = forward(jnp.stack([advect, bulk_term]))
    vortex = inverse(jnp.stack(vortex_hat, axis=1))
    flow_side = forward(momentum(velocity, vortex, leading[0:3], potential))
    nonlinear = jnp.concatenate([phase_side, flow_side], axis=1)
    mean_mode = (wave_x == 0) & (wave_y == 0) & (wave_z == 0)
    advect_hat = jnp.where(mean_mode, 0.0, nonlinear[:, 0])
    bulk_hat = nonlinear[:, 1]
    stable_part = 1.0 / time_step + mobility * stabilizer * squared
    new_phase = (stable_part * coeff_phase - advect_hat - mobility * squared * bulk_hat) / (
        stable_part + mobility * epsilon * epsilon * squared * squared
    )
    viscous = 1.0 / time_step + squared / reynolds
    unprojected = [
        (spectra[:, 1 + j] / time_step + nonlinear[:, 2 + j]) / viscous for j in range(3)
    ]
    normal_part = (
        wave_x * unprojected[0] + wave_y * unprojected[1] + wave_z * unprojected[2]
    ) / jnp.maximum(squared, 1.0)
    waves = [wave_x, wave_y, wave_z]
    new_flow = [unprojected[j] - waves[j] * normal_part for j in range(3)]
    result = inverse(jnp.stack([new_phase] + new_flow, axis=1))
    return (result[0], result[1:4])


def tables(cols, rows, rows_y, planes):
    total_z = planes * rows
    half_z = 3 * total_z // 8
    modes_z = 2 * half_z
    kx_row = KC // rows

    def pair(first, second, period):
        residue = first[:, None] * second[None, :] % period
        angles = residue.astype(np.float32) * np.float32(2.0 * math.pi / period)
        return [np.cos(angles).astype(ml_dtypes.bfloat16), np.sin(angles).astype(ml_dtypes.bfloat16)]

    cos_x, sin_x = pair(np.arange(KC), np.arange(NX), NX)
    cos_y, sin_y = pair(np.arange(NY), np.arange(KY) - KC, NY)
    cos_z, sin_z = pair(np.arange(total_z), np.arange(modes_z) - half_z, total_z)
    order = np.arange(KC).reshape(cols, rows, kx_row // cols).transpose(1, 0, 2).reshape(KC)
    x_table = np.stack([cos_x[order], -sin_x[order]]).reshape(2, rows, kx_row // 2, 2, NX)
    x_table = x_table.transpose(1, 0, 3, 2, 4).reshape(2 * KC, NX)
    y_forward = np.concatenate([cos_y, sin_y], axis=1)
    cz, sz = (t.reshape(rows, planes, modes_z) for t in (cos_z, sin_z))
    z_forward = np.stack([np.stack([cz, sz], 1), np.stack([-sz, cz], 1)])
    z_forward = z_forward.transpose(0, 4, 1, 2, 3).reshape(2 * modes_z, 2 * total_z)
    z_inverse = np.stack([np.stack([cz, -sz], 2), np.stack([sz, cz], 2)], 1)
    z_inverse = z_inverse.reshape(2 * total_z, 2 * modes_z)
    z_rotated = np.concatenate([z_inverse[:, modes_z:], -z_inverse[:, :modes_z]], axis=1)
    x_wide = np.stack([cos_x, -sin_x]).reshape(2, cols, kx_row * rows // cols, NX)
    x_wide = x_wide.transpose(1, 0, 2, 3).reshape(2 * KC, NX)
    made = (x_wide, y_forward, z_forward, z_inverse, z_rotated, x_table)
    return [jnp.asarray(t.astype(ml_dtypes.bfloat16)) for t in made]


def dot(first, second, dims=((1,), (0,))):
    return lax.dot_general(first, second, (dims, ((), ())), preferred_element_type=jnp.float32)


LANES = 128


def fast_device(sizes, phase, velocity):
    cols, rows, rows_y, planes = sizes
    total_z = planes * rows
    half_z = 3 * total_z // 8
    modes_z = 2 * half_z
    kx_row = KC // rows
    kx_own = kx_row // cols
    pairs = kx_row // 2
    points = rows_y * planes
    row_lanes = kx_row * rows_y
    col_lanes = kx_own * rows_y
    own = kx_own * modes_z
    scale_inv = 1.0 / (NX * NY * total_z)
    made_tables = tables(cols, rows, rows_y, planes)
    f32, bf16 = jnp.float32, jnp.bfloat16
    forward_count, derived_count, derived_lines, final_count = 7, 7, 6, 3
    row_count = forward_count + derived_count
    col_count = forward_count + derived_lines
    kx_col = kx_own * rows
    wide_lanes = kx_own * KY

    def partner(me, d, size):
        if size & (size - 1):
            return lax.rem(me + d, size)
        peer, bit = 0, 1
        while bit < size:
            mine = (me // bit) % 2
            peer = peer + bit * (1 - mine if d & bit else mine)
            bit *= 2
        return peer

    def exchange(axis, size, src, dst, send, recv):
        me = lax.axis_index(axis)

        def copy(f, d):
            peer = partner(me, d, size)
            return pltpu.make_async_remote_copy(
                src_ref=src.at[f, peer],
                dst_ref=dst.at[f, me],
                send_sem=send.at[f, d - 1],
                recv_sem=recv.at[f, d - 1],
                device_id={axis: peer},
                device_id_type=pl.DeviceIdType.MESH,
            )

        def start(f):
            for d in reversed(range(1, size)):
                copy(f, d).start()
            dst[f, me] = src[f, me]

        def arrived(f):
            for d in range(1, size):
                copy(f, d).wait_recv()

        def sent(f):
            for d in range(1, size):
                copy(f, d).wait_send()

        return start, arrived, sent

    def greet():
        barrier = pltpu.get_barrier_semaphore()
        for axis, size in (("col", cols), ("row", rows)):
            for d in range(1, size):
                peer = lax.rem(lax.axis_index(axis) + d, size)
                pl.semaphore_signal(
                    barrier, inc=1, device_id={axis: peer}, device_id_type=pl.DeviceIdType.MESH
                )

    def greeted():
        pl.semaphore_wait(pltpu.get_barrier_semaphore(), cols + rows - 2)

    def swap_halves(first, second):
        half = LANES // 2
        low = jnp.concatenate([first[:, :half], second[:, :half]], axis=1)
        high = jnp.concatenate([first[:, half:], second[:, half:]], axis=1)
        return low, high

    def body(*refs):
        phase_in, flow_in = refs[:2]
        table_in = refs[2:8]
        phase_out, flow_out = refs[8:10]
        (
            row_src, row_dst, col_src, col_dst, thin_src, thin_dst, wide_src, wide_dst,
            fields, lines, derived, coeff, ready,
            xw_tab, yf_tab, zf_tab, zi_tab, zr_tab, x_tab, yi_tab,
            row_send, row_recv, col_send, col_recv, thin_send, thin_recv, wide_send, wide_recv,
            load_sem, table_sem, store_sem,
        ) = refs[10:]
        table_refs = (xw_tab, yf_tab, zf_tab, zi_tab, zr_tab, x_tab)
        row_start, row_arrived, row_sent = exchange("row", rows, row_src, row_dst, row_send, row_recv)
        col_start, col_arrived, col_sent = exchange("col", cols, col_src, col_dst, col_send, col_recv)
        thin_start, thin_arrived, thin_sent = exchange(
            "row", rows, thin_src, thin_dst, thin_send, thin_recv
        )
        wide_start, wide_arrived, wide_sent = exchange(
            "col", cols, wide_src, wide_dst, wide_send, wide_recv
        )

        def load(j, z):
            source = phase_in.at[:, z, :] if j == 0 else flow_in.at[j - 1, :, z, :]
            target = fields.at[j, pl.ds(z * rows_y, rows_y), :]
            return pltpu.make_async_copy(source, target, load_sem.at[j, z])

        def store(j, z):
            target = phase_out.at[:, z, :] if j == 0 else flow_out.at[j - 1, :, z, :]
            source = derived.at[j, pl.ds(z * rows_y, rows_y), :]
            return pltpu.make_async_copy(source, target, store_sem.at[j, z])

        def table_copy(k):
            return pltpu.make_async_copy(table_in[k], table_refs[k], table_sem.at[k])

        row_kx = lax.axis_index("row") * kx_own
        own_kx = lax.axis_index("col") * kx_col + row_kx

        def x_forward(f):
            made = dot(x_tab[...], lines[lax.rem(f, 5)], ((1,), (1,)))
            for r in range(rows):
                parts = []
                for p in range(2):
                    base = (r * 2 + p) * kx_row
                    even = made[base : base + pairs]
                    odd = made[base + pairs : base + kx_row]
                    planes_made = []
                    for j in range(planes // 2):
                        at = slice(j * LANES, (j + 1) * LANES)
                        planes_made.extend(swap_halves(even[:, at], odd[:, at]))
                    parts.append(jnp.swapaxes(jnp.stack(planes_made), 0, 1))
                both = jnp.concatenate(parts, axis=1).astype(bf16)
                for k in range(pairs):
                    row_src[f - 1, r, :, k * LANES : (k + 1) * LANES] = both[k]
            row_start(f - 1)

        def x_inverse(h):
            row_arrived(h)
            made = []
            for r in range(rows):
                whole_lines = row_dst[h, r].astype(f32)
                tiles = jnp.stack([whole_lines[:, k * LANES : (k + 1) * LANES] for k in range(pairs)])
                for p in range(2):
                    by_plane = jnp.swapaxes(tiles[:, p * planes : (p + 1) * planes], 0, 1)
                    even, odd = [], []
                    for j in range(planes // 2):
                        low, high = swap_halves(by_plane[2 * j], by_plane[2 * j + 1])
                        even.append(low)
                        odd.append(high)
                    made.append(jnp.concatenate(even, axis=1))
                    made.append(jnp.concatenate(odd, axis=1))
            gathered = jnp.concatenate(made, axis=0).astype(bf16)
            return dot(gathered, x_tab[...], ((0,), (0,)))

        def z_forward(f):
            row_arrived(f - 1)
            stacked = row_dst[f - 1].reshape(2 * total_z, row_lanes)
            made = dot(zf_tab[...], stacked).astype(bf16)
            for c in range(cols):
                col_src[f - 1, c] = made[:, c * col_lanes : (c + 1) * col_lanes]
            col_start(f - 1)

        def joined(g):
            return jnp.concatenate([col_dst[g, c] for c in range(cols)], axis=1)

        def row_emit(h, made):
            made = made.astype(bf16)
            for r in range(rows):
                row_src[h, r] = made[r * 2 * planes : (r + 1) * 2 * planes]
            row_start(h)

        def inverse_table():
            for t in range(2):
                part = yf_tab[:, t * KY : (t + 1) * KY].astype(f32)
                yi_tab[:, t * NY : (t + 1) * NY] = part.T.astype(bf16)

        def wide_x(slot, line):
            made = dot(xw_tab[...], lines[line], ((1,), (1,))).astype(bf16)
            wide_src[slot] = made.reshape(cols, 2 * kx_col, points)

        def wide_y(slot):
            wide_arrived(slot)
            lhs = jnp.concatenate(
                [
                    jnp.concatenate(
                        [wide_dst[slot, c, :, z * rows_y : (z + 1) * rows_y] for c in range(cols)],
                        axis=1,
                    )
                    for z in range(planes)
                ],
                axis=0,
            )
            made = dot(lhs, yf_tab[...]).reshape(planes, 2 * kx_col, 2 * KY)
            first, second = made[:, :kx_col], made[:, kx_col:]
            real = jnp.swapaxes(first[:, :, :KY] + second[:, :, KY:], 0, 1)
            imag = jnp.swapaxes(second[:, :, :KY] - first[:, :, KY:], 0, 1)
            both = jnp.concatenate([real, imag], axis=1).astype(bf16)
            for k in range(kx_col):
                r, a = k // kx_own, k % kx_own
                thin_src[slot, r, :, a * KY : (a + 1) * KY] = both[k]
            thin_start(slot)

        def wide_z(slot, f):
            thin_arrived(slot)
            stacked = thin_dst[slot].reshape(2 * total_z, wide_lanes)
            made = dot(zf_tab[...], stacked) * scale_inv
            for p in range(2):
                for a in range(kx_own):
                    coeff[f, p, a * modes_z : (a + 1) * modes_z, :] = made[
                        p * modes_z : (p + 1) * modes_z, a * KY : (a + 1) * KY
                    ]

        def last_z():
            parts = []
            for p in range(2):
                parts.append(
                    jnp.concatenate(
                        [coeff[0, p, a * modes_z : (a + 1) * modes_z, :] for a in range(kx_own)], axis=1
                    )
                )
            made = dot(zi_tab[...], jnp.concatenate(parts, axis=0).astype(bf16)).astype(bf16)
            for r in range(rows):
                thin_src[0, r] = made[r * 2 * planes : (r + 1) * 2 * planes]
            thin_start(0)

        def last_y():
            thin_arrived(0)
            lhs = jnp.concatenate(
                [
                    thin_dst[0, r, :, a * KY : (a + 1) * KY]
                    for r in range(rows)
                    for a in range(kx_own)
                ],
                axis=0,
            )
            made = dot(lhs, yi_tab[...]).reshape(kx_col, 2 * planes, 2 * NY)
            first, second = made[:, :planes], made[:, planes:]
            real = jnp.swapaxes(first[:, :, :NY] - second[:, :, NY:], 0, 1)
            imag = jnp.swapaxes(first[:, :, NY:] + second[:, :, :NY], 0, 1)
            both = jnp.concatenate([real, imag], axis=1).astype(bf16)
            for c in range(cols):
                wide_src[0, c] = jnp.concatenate(
                    [both[z, :, c * rows_y : (c + 1) * rows_y] for z in range(planes)], axis=1
                )
            wide_start(0)

        def last_x():
            wide_arrived(0)
            gathered = wide_dst[0].reshape(2 * KC, points)
            return dot(gathered, xw_tab[...], ((0,), (0,)))

        def z_inverse(g, h):
            col_arrived(g)
            row_emit(h, dot(zi_tab[...], joined(g)))

        def y_forward(f):
            col_arrived(f - 1)
            lhs = jnp.concatenate(
                [
                    jnp.concatenate(
                        [col_dst[f - 1, c, :, a * rows_y : (a + 1) * rows_y] for c in range(cols)], axis=1
                    )
                    for a in range(kx_own)
                ],
                axis=0,
            )
            made = dot(lhs, yf_tab[...]).reshape(kx_own, 2 * modes_z, 2 * KY)
            first, second = made[:, :modes_z], made[:, modes_z:]
            real = first[:, :, :KY] + second[:, :, KY:]
            imag = second[:, :, :KY] - first[:, :, KY:]
            coeff[f, 0] = real.reshape(own, KY) * scale_inv
            coeff[f, 1] = imag.reshape(own, KY) * scale_inv

        def y_inverse(e, g):
            made = dot(ready[e], yi_tab[...])
            first, second = made[:own], made[own:]
            real = (first[:, :NY] - second[:, NY:]).reshape(kx_own, modes_z, NY)
            imag = (first[:, NY:] + second[:, :NY]).reshape(kx_own, modes_z, NY)
            both = jnp.concatenate([real, imag], axis=1).astype(bf16)
            for c in range(cols):
                col_src[g, c] = jnp.concatenate(
                    [both[a, :, c * rows_y : (c + 1) * rows_y] for a in range(kx_own)], axis=1
                )
            col_start(g)

        block = 2 * modes_z

        def spectral(work):
            def step(i, carry):
                base = pl.multiple_of(i * block, block)
                at = pl.ds(base, block)
                row = lax.broadcasted_iota(jnp.int32, (block, KY), 0)
                upper = row >= modes_z
                kx = own_kx + 2 * i + jnp.where(upper, 1, 0)
                kz = jnp.where(upper, row - modes_z, row) - half_z
                ky = lax.broadcasted_iota(jnp.int32, (block, KY), 1) - KC
                weight = jnp.where(kx == 0, 1.0, 2.0)
                mean_mode = (kx == 0) & (ky == 0) & (kz == 0)
                wx, wy = kx.astype(f32), ky.astype(f32)
                wz = kz.astype(f32) * (NX / total_z)
                k2 = wx * wx + wy * wy + wz * wz

                def get(f):
                    return coeff[f, 0, at, :], coeff[f, 1, at, :]

                def put(e, real, imag):
                    if e is None:
                        coeff[0, 0, at, :] = real * weight
                        coeff[0, 1, at, :] = imag * weight
                        return
                    ready[e, at, :] = (real * weight).astype(bf16)
                    ready[e, pl.ds(pl.multiple_of(own + base, block), block), :] = (
                        imag * weight
                    ).astype(bf16)

                work(get, put, wx, wy, wz, k2, mean_mode)
                return carry

            lax.fori_loop(0, own // block, step, 0)

        def derive_phase(get, put, wx, wy, wz, k2, mean_mode):
            real, imag = get(0)
            put(0, real, imag)
            put(1, -(wy * imag), wy * real)
            put(2, -k2 * real, -k2 * imag)

        def derive_vortex(get, put, wx, wy, wz, k2, mean_mode):
            w = [wx, wy, wz]
            got = [get(1 + j) for j in range(3)]
            for e, j in ((3, 2), (4, 1), (5, 0)):
                p, q = (j + 1) % 3, (j + 2) % 3
                real = -(w[p] * got[q][1] - w[q] * got[p][1])
                put(e, real, w[p] * got[q][0] - w[q] * got[p][0])

        def solve_phase(get, put, wx, wy, wz, k2, mean_mode):
            old, bulk_hat, advect_hat = get(0), get(4), get(5)
            stable = 1.0 / time_step + mobility * stabilizer * k2
            below = stable + mobility * epsilon * epsilon * k2 * k2
            made = []
            for p in range(2):
                kept = jnp.where(mean_mode, 0.0, advect_hat[p])
                made.append((stable * old[p] - kept - mobility * k2 * bulk_hat[p]) / below)
            put(0, made[0], made[1])

        forcing_slot = (8, 6, 7)

        def solve_flow(get, put, wx, wy, wz, k2, mean_mode):
            viscous = 1.0 / time_step + k2 / reynolds
            largest = jnp.maximum(k2, 1.0)
            w = [wx, wy, wz]
            old = [get(1 + j) for j in range(3)]
            added = [get(forcing_slot[j]) for j in range(3)]
            made = [[], [], []]
            for p in range(2):
                free = [(old[j][p] / time_step + added[j][p]) / viscous for j in range(3)]
                normal = (wx * free[0] + wy * free[1] + wz * free[2]) / largest
                for j in range(3):
                    made[j].append(free[j] - w[j] * normal)
            for j in range(3):
                put(1 + j if j < 2 else None, made[j][0], made[j][1])

        cut = 32

        def pointwise(work):
            def step(i, carry):
                work(pl.ds(pl.multiple_of(i * cut, cut), cut))
                return carry

            lax.fori_loop(0, points // cut, step, 0)

        def loop(begin, end, work):
            def step(i, carry):
                work(i)
                return carry

            lax.fori_loop(begin, end, step, 0)

        for z in range(planes):
            load(0, z).start()
        for k in range(len(table_refs)):
            table_copy(k).start()
        for j in range(1, 4):
            for z in range(planes):
                load(j, z).start()
        greet()

        def cast(f):
            def work(at):
                lines[f, at, :] = fields[f, at, :].astype(bf16)

            pointwise(work)

        def bring(f):
            for z in range(planes):
                load(f, z).wait()
            cast(f)

        def make_bulk(at):
            c = fields[0, at, :]
            lines[4, at, :] = (c * c * c - c).astype(bf16)

        def send_derived(e):
            y_inverse(e, forward_count + e)

        table_copy(0).wait()
        bring(0)
        wide_x(0, 0)
        greeted()
        wide_start(0)
        for k in range(1, len(table_refs)):
            table_copy(k).wait()
        for j in range(1, 4):
            bring(j)
        loop(1, 4, x_forward)
        inverse_table()
        pointwise(make_bulk)
        loop(1, 3, z_forward)
        wide_y(0)
        x_forward(4)
        z_forward(3)
        wide_z(0, 0)
        spectral(derive_phase)
        send_derived(0)
        loop(1, 3, y_forward)
        send_derived(1)
        y_forward(3)
        spectral(derive_vortex)
        loop(2, 5, send_derived)

        g0 = forward_count
        h0 = forward_count

        def phase_planes():
            col_arrived(g0)
            data = joined(g0)
            at_lane = lax.broadcasted_iota(jnp.int32, (1, row_lanes), 1)
            owner = at_lane // col_lanes
            lane_kx = owner * (kx_col - kx_own) + at_lane // rows_y + row_kx
            row_emit(h0, dot(zr_tab[...], data) * lane_kx.astype(f32))
            row = lax.broadcasted_iota(jnp.int32, (2 * modes_z, 1), 0)
            kz = jnp.where(row >= modes_z, row - modes_z, row) - half_z
            scaled = (data.astype(f32) * (kz.astype(f32) * (NX / total_z))).astype(bf16)
            row_emit(h0 + 1, dot(zr_tab[...], scaled))

        def to_field(i):
            derived[i] = x_inverse(h0 + i)

        def make_advect(at):
            lines[0, at, :] = (
                fields[1, at, :] * derived[0, at, :]
                + fields[2, at, :] * derived[2, at, :]
                + fields[3, at, :] * derived[1, at, :]
            ).astype(bf16)

        gradient_at = (0, 2, 1)
        vortex_at = (6, 5, 4)

        def make_forcing(which):
            def work(at):
                c = fields[0, at, :]
                potential = c * c * c - c - epsilon * epsilon * derived[3, at, :]
                for j in which:
                    p, q = (j + 1) % 3, (j + 2) % 3
                    lines[(3, 1, 2)[j], at, :] = (
                        fields[1 + p, at, :] * derived[vortex_at[q], at, :]
                        - fields[1 + q, at, :] * derived[vortex_at[p], at, :]
                        + potential * derived[gradient_at[j], at, :]
                    ).astype(bf16)

            return work

        phase_planes()
        send_derived(5)
        z_inverse(g0 + 1, h0 + 2)
        loop(0, 2, to_field)
        z_inverse(g0 + 2, h0 + 3)
        to_field(2)
        pointwise(make_advect)
        x_forward(5)
        z_inverse(g0 + 3, h0 + 4)
        to_field(3)
        z_forward(4)
        z_forward(5)
        z_inverse(g0 + 4, h0 + 5)
        to_field(4)
        z_inverse(g0 + 5, h0 + 6)
        to_field(5)
        pointwise(make_forcing((0,)))
        wide_x(1, 3)
        wide_start(1)
        to_field(6)
        pointwise(make_forcing((1, 2)))
        loop(6, 8, x_forward)
        loop(6, 8, z_forward)
        loop(4, 6, y_forward)
        spectral(solve_phase)
        loop(0, final_count, row_sent)
        loop(0, final_count, col_sent)
        thin_sent(0)
        wide_sent(0)
        y_inverse(0, 0)
        wide_y(1)
        wide_z(1, 8)
        loop(6, 8, y_forward)
        spectral(solve_flow)
        last_z()
        def send_flow(e):
            y_inverse(e, e)

        loop(1, final_count, send_flow)
        last_y()

        z_inverse(0, 0)

        def finish(j):
            z_inverse(j + 1, j + 1)
            derived[j] = x_inverse(j)

        def emit(j):
            for z in range(planes):
                store(j, z).start()

        loop(0, 2, finish)
        emit(0)
        emit(1)
        derived[2] = x_inverse(2)
        emit(2)
        derived[3] = last_x()
        emit(3)
        loop(0, row_count, row_sent)
        loop(0, col_count, col_sent)
        loop(0, 2, thin_sent)
        loop(0, 2, wide_sent)
        for j in range(4):
            for z in range(planes):
                store(j, z).wait()

    sems = pltpu.SemaphoreType.DMA
    row_shape = (row_count, rows, 2 * planes, row_lanes)
    col_shape = (col_count, cols, 2 * modes_z, col_lanes)
    thin_shape = (2, rows, 2 * planes, wide_lanes)
    wide_shape = (2, cols, 2 * kx_col, points)
    scratch = []
    for shape in (row_shape, col_shape, thin_shape, wide_shape):
        scratch += [pltpu.VMEM(shape, bf16), pltpu.VMEM(shape, bf16)]
    scratch += [
        pltpu.VMEM((4, points, NX), f32),
        pltpu.VMEM((5, points, NX), bf16),
        pltpu.VMEM((derived_count, points, NX), f32),
        pltpu.VMEM((9, 2, own, KY), f32),
        pltpu.VMEM((derived_lines, 2 * own, KY), bf16),
    ]
    scratch += [pltpu.VMEM(t.shape, bf16) for t in made_tables]
    scratch += [pltpu.VMEM((KY, 2 * NY), bf16)]
    for shape, size in ((row_shape, rows), (col_shape, cols), (thin_shape, rows), (wide_shape, cols)):
        scratch += [sems((shape[0], size - 1)), sems((shape[0], size - 1))]
    scratch += [sems((4, planes)), sems((len(made_tables),)), sems((4, planes))]
    hbm = pl.BlockSpec(memory_space=pltpu.HBM)
    out_shape = [
        jax.ShapeDtypeStruct(phase.shape, f32),
        jax.ShapeDtypeStruct(velocity.shape, f32),
    ]
    result = pl.pallas_call(
        body,
        in_specs=[hbm] * (2 + len(made_tables)),
        out_specs=[hbm, hbm],
        out_shape=out_shape,
        scratch_shapes=scratch,
        compiler_params=pltpu.CompilerParams(
            collective_id=0, has_side_effects=True, vmem_limit_bytes=67_043_328
        ),
        cost_estimate=pl.CostEstimate(
            flops=8_000_000_000, bytes_accessed=1 << 23, transcendentals=0
        ),
    )(phase, velocity, *made_tables)

    cuts = 2
    part = rows_y // cuts

    def deliver(phase_in, flow_in, phase_out, flow_out, held, load_sem, store_sem):
        def copies(j, k):
            at = pl.ds(k * part, part)
            source = phase_in.at[at] if j == 0 else flow_in.at[j - 1, at]
            target = phase_out.at[at] if j == 0 else flow_out.at[j - 1, at]
            load = pltpu.make_async_copy(source, held.at[j, at], load_sem.at[j, k])
            return load, pltpu.make_async_copy(held.at[j, at], target, store_sem.at[j, k])

        for j in range(4):
            for k in range(cuts):
                copies(j, k)[0].start()
        for j in range(4):
            for k in range(cuts):
                copies(j, k)[0].wait()
                copies(j, k)[1].start()
        for j in range(4):
            for k in range(cuts):
                copies(j, k)[1].wait()

    return tuple(
        pl.pallas_call(
            deliver,
            in_specs=[hbm, hbm],
            out_specs=[hbm, hbm],
            out_shape=out_shape,
            scratch_shapes=[
                pltpu.VMEM((4,) + phase.shape, f32), sems((4, cuts)), sems((4, cuts)),
            ],
            compiler_params=pltpu.CompilerParams(vmem_limit_bytes=67_043_328),
            cost_estimate=pl.CostEstimate(
                flops=1_000_000, bytes_accessed=1 << 23, transcendentals=0
            ),
        )(*result)
    )


def solution(mesh):
    cols, rows = mesh.shape["col"], mesh.shape["row"]

    def on_device(phase, velocity):
        rows_y, planes = phase.shape[0], phase.shape[1]
        kx_own = KC // (rows * cols)
        modes_z = 2 * (3 * planes * rows // 8)
        aligned = planes == 8 and 2 * rows_y == LANES and cols % 2 == 0
        exact = KC == kx_own * rows * cols and kx_own % 2 == 0 and modes_z % 8 == 0
        if aligned and exact:
            return fast_device((cols, rows, rows_y, planes), phase, velocity)
        return plain_device(phase, velocity)

    return jax.shard_map(
        on_device,
        mesh=mesh,
        in_specs=(P("col", "row", None), P(None, "col", "row", None)),
        out_specs=(P("col", "row", None), P(None, "col", "row", None)),
        check_vma=False,
    )
```
